32 devices in a mesh: wide: 8 (over z, y), narrow: 4 (over x, core).
Axes of the slice: x: 2, y: 2, z: 4, core: 2. Of those that a mesh axis runs over, the one named last changes fastest.
Arguments:
- checkpoint_slots: float32 [4, 2, 256, 4096], P('narrow', None, 'wide'), may hold values from 0 to 2
- owner_slot: int32 [2], replicated, may hold values from 0 to 3
- row_velocity: float32 [256, 4096], P('wide', 'narrow'), may hold values from -0.4 to 0.4
- column_velocity: float32 [256, 4096], P('wide', 'narrow'), may hold values from -0.4 to 0.4
- land_sea: int32 [256, 4096], P('wide', 'narrow'), may hold values 0 or 1
- layer_class: int32 [2], replicated, may hold values from 0 to 3
- class_speed: float32 [4], replicated, may hold values from 0.05 to 0.6
- final_adjoint: float32 [2, 256, 4096], P(None, 'wide', 'narrow'), may hold values from -6 to 6
- deposit_weight: float32 [256, 4096], P('wide', 'narrow'), may hold values from -6 to 6
Outputs:
- initial_adjoint: float32 [2, 256, 4096], P(None, 'wide', 'narrow')
The draws below stay inside these ranges and needn't reach their ends.
All inputs are finite; a program needn't handle non-finite values. No bound on the sum of `land_sea` on one device may be relied on, other than what follows from the above.
Results may differ from the reference program's by a relative error of at most 0.00002.
Values sent between devices are 32-bit elements; how exact they have to be, the bound alone decides.
A program may use at most 64 MiB of HBM per device.

```python
import math
import jax
import jax.numpy as jnp
from jax import lax

LAYERS = 2
CLASSES = 4
STEPS = 3
NX = 256
NY = 4096
N_NARROW = 4


def with_ends(values, rng, low, top_value):
    shape = values.shape
    spot = [jax.random.randint(jax.random.fold_in(rng, axis), (), 0, shape[axis]) for axis in range(len(shape))]
    values = values.at[tuple(spot)].set(low)
    longest = shape.index(max(shape))
    spot[longest] = (spot[longest] + 1) % shape[longest]
    return values.at[tuple(spot)].set(top_value)


def block_levels(stream_key, dims, pieces, smallest, largest):
    gain, own = 1.0, jax.random.fold_in(stream_key, 6)
    for dim, shards_of in pieces:
        draws = jnp.exp(jax.random.uniform(jax.random.fold_in(own, dim), (shards_of,), jnp.float32, smallest / len(pieces), largest / len(pieces)))
        gain = gain * jnp.repeat(draws, dims[dim] // shards_of).reshape([-1 if axis == dim else 1 for axis in range(len(dims))])
    return gain


def gaussian(stream_key, shape, spread, reach, cuts=(), kind=jnp.bfloat16):
    loudness = block_levels(stream_key, shape, cuts, -0.22, 0.18) if cuts else 1.0
    values = jax.random.normal(stream_key, shape, jnp.float32) * spread * loudness
    return jnp.minimum(jnp.maximum(values, -reach), reach).astype(kind)


def setup_inputs(seed: int = 0) -> dict:
    splits = jax.random.split(jax.random.key(seed), 10)
    return {
        "checkpoint_slots": jnp.clip(2.0 * jax.random.uniform(splits[0], (N_NARROW, LAYERS, NX, NY), jnp.float32) ** block_levels(splits[0], (N_NARROW, LAYERS, NX, NY), ((0, 4), (2, 8)), -0.2, 0.2), 0.0, 2.0),
        "owner_slot": jax.random.randint(splits[1], (LAYERS,), 0, N_NARROW).astype(jnp.int32),
        "row_velocity": jnp.clip(jax.random.uniform(splits[2], (NX, NY), jnp.float32, -0.4, 0.4) * block_levels(splits[2], (NX, NY), ((0, 8), (1, 4)), -0.4, 0.0), -0.4, 0.4),
        "column_velocity": jnp.clip(jax.random.uniform(splits[3], (NX, NY), jnp.float32, -0.4, 0.4) * block_levels(splits[3], (NX, NY), ((0, 8), (1, 4)), -0.4, 0.0), -0.4, 0.4),
        "land_sea": with_ends((jax.random.randint(splits[4], (NX, NY), 0, 8) < 7).astype(jnp.int32), jax.random.fold_in(splits[4], 1), 0, 1),
        "layer_class": jax.random.randint(splits[5], (LAYERS,), 0, CLASSES).astype(jnp.int32),
        "class_speed": jnp.clip(jnp.exp(jax.random.uniform(splits[6], (CLASSES,), jnp.float32, math.log(0.05), math.log(0.6))), 0.05, 0.6),
        "final_adjoint": gaussian(splits[7], (LAYERS, NX, NY), 1.0, 6.0, ((1, 8), (2, 4)), jnp.float32),
        "deposit_weight": gaussian(splits[8], (NX, NY), 1.0, 6.0, ((0, 8), (1, 4)), jnp.float32),
    }


def stencil_weights(velocity):
    forward_part = jnp.maximum(velocity, 0.0)
    backward_part = jnp.minimum(velocity, 0.0)
    fsquare = forward_part * forward_part
    bsquare = backward_part * backward_part
    return [0.5 * fsquare - 0.5 * forward_part, 2.0 * forward_part - fsquare, 0.5 * fsquare - 1.5 * forward_part + 0.5 * bsquare + 1.5 * backward_part, -2.0 * backward_part - bsquare, 0.5 * bsquare + 0.5 * backward_part]

def advect(padded, row_weights, column_weights):
    height = padded.shape[1]
    breadth = padded.shape[2]
    result = padded[:, 2:height - 2, 2:breadth - 2]
    for offset in range(-2, 3):
        row_term = row_weights[offset + 2][2:height - 2, 2:breadth - 2]
        column_term = column_weights[offset + 2][2:height - 2, 2:breadth - 2]
        result = result + row_term * padded[:, 2 + offset:height - 2 + offset, 2:breadth - 2]
        result = result + column_term * padded[:, 2:height - 2, 2 + offset:breadth - 2 + offset]
    return result

def settle(advected, speeds, sea_mask):
    flux = speeds[:, None, None] * advected / (1.0 + advected * advected)
    above = jnp.concatenate([jnp.zeros_like(flux[:1]), flux[:-1]], 0)
    return ((advected - flux + above) * sea_mask, flux[-1] * sea_mask)

def layer_speeds(layer_class, class_speed):
    classes = jnp.arange(class_speed.shape[0], dtype=jnp.int32)
    return lax.optimization_barrier(jnp.sum(jnp.where(layer_class[:, None] == classes[None, :], class_speed[None, :], 0.0), axis=1))

def reference(checkpoint_slots, owner_slot, row_velocity, column_velocity, land_sea, layer_class, class_speed, final_adjoint, deposit_weight):
    slot_ids = jnp.arange(checkpoint_slots.shape[0], dtype=jnp.int32)
    chosen = owner_slot.astype(jnp.int32)[None, :, None, None] == slot_ids[:, None, None, None]
    start_state = lax.optimization_barrier(jnp.sum(jnp.where(chosen, checkpoint_slots, 0.0), axis=0))
    speeds = layer_speeds(layer_class, class_speed)
    sea_mask = land_sea.astype(jnp.float32)
    row_weights = stencil_weights(jnp.pad(row_velocity, 2))
    column_weights = stencil_weights(jnp.pad(column_velocity, 2))

    def forward(current):
        deposit = jnp.zeros_like(sea_mask)
        for step_index in range(STEPS):
            padded = jnp.pad(current, ((0, 0), (2, 2), (2, 2)))
            advected = advect(padded, row_weights, column_weights)
            current, bottom = settle(advected, speeds, sea_mask)
            deposit = deposit + bottom
        return (current, deposit)
    unused, pullback = jax.vjp(forward, start_state)
    initial, = pullback((final_adjoint, deposit_weight))
    return initial
```

```python
import functools

import jax
import jax.numpy as jnp
from jax import lax
from jax.experimental import pallas as pl
from jax.experimental.pallas import tpu as pltpu
from jax.sharding import PartitionSpec as P

STEPS = 3
LANES = 128
ROWS = 8
REACH = 2 * STEPS
OFFSETS = (-2, -1, 1, 2)
MESH = pl.DeviceIdType.MESH
VMEM_BYTES = 67043328


def stencil_weights(velocity):
    p = jnp.maximum(velocity, 0.0)
    q = jnp.minimum(velocity, 0.0)
    pp = p * p
    qq = q * q
    return [
        0.5 * pp - 0.5 * p,
        2.0 * p - pp,
        0.5 * pp - 1.5 * p + 0.5 * qq + 1.5 * q,
        -2.0 * q - qq,
        0.5 * qq + 0.5 * q,
    ]


def kernel(
    group_wide,
    group,
    owner_hbm,
    class_hbm,
    speed_hbm,
    slots_hbm,
    row_velocity_hbm,
    column_velocity_hbm,
    sea_hbm,
    final_hbm,
    deposit_hbm,
    out_ref,
    owner_ref,
    class_ref,
    speed_ref,
    sea_ref,
    fixed,
    fixed_col,
    given,
    given_col,
    mine,
    give,
    near,
    mixed,
    far,
    field,
    field_col,
    slope,
    grad,
    wr,
    wc,
    wr_back,
    wc_back,
    centre,
    round_send,
    round_recv,
    load_sems,
    slot_sems,
    near_sems,
    far_sems,
    fixed_sems,
    given_sems,
    col_sems,
    row_sems,
    corner_sems,
    round_sems,
):
    layers, height, breadth = out_ref.shape
    pair = 2
    chips = group // pair
    w = lax.axis_index("wide")
    n = lax.axis_index("narrow")
    chip = lax.div(n, pair)
    core = lax.rem(n, pair)
    width = breadth + LANES
    own_blocks = height // ROWS
    extended = height + 2 * ROWS
    all_blocks = list(range(own_blocks + 2))
    edge = (slice(0, LANES), slice(breadth - LANES, breadth))
    side_block = slice(breadth, width)
    own = slice(ROWS, ROWS + height)

    has_row = (w > 0, w < group_wide - 1)
    has_col = (n > 0, n < group - 1)
    row_device = ((w - 1, n), (w + 1, n))
    col_device = ((w, n - 1), (w, n + 1))
    partner = (w, chip * pair + (pair - 1 - core))
    order = [lax.rem(chip + by, chips) for by in range(1, chips)] + [chip]
    parts = (
        slice(0, ROWS),
        slice(height - ROWS, height),
        slice(ROWS, height - ROWS),
    )

    def columns_of(device):
        return pl.ds(pl.multiple_of(device * breadth, LANES), breadth)

    def remote(src, dst, send_sem, recv_sem, device):
        return pltpu.make_async_remote_copy(
            src_ref=src,
            dst_ref=dst,
            send_sem=send_sem,
            recv_sem=recv_sem,
            device_id=device,
            device_id_type=MESH,
        )

    small = [
        pltpu.make_async_copy(source, target, load_sems.at[i])
        for i, (source, target) in enumerate(
            [
                (owner_hbm, owner_ref),
                (class_hbm, class_ref),
                (speed_hbm, speed_ref),
                (sea_hbm, sea_ref),
                (row_velocity_hbm, fixed.at[0, own, 0:breadth]),
                (column_velocity_hbm, fixed.at[1, own, 0:breadth]),
                (final_hbm, given.at[0:layers, own, 0:breadth]),
                (deposit_hbm, given.at[layers, own, 0:breadth]),
            ]
        )
    ]
    give_loads = [
        pltpu.make_async_copy(
            slots_hbm.at[0, :, :, columns_of(order[step] * pair + (pair - 1 - core))],
            give.at[step],
            slot_sems.at[0, step],
        )
        for step in range(chips)
    ]
    mine_loads = [
        pltpu.make_async_copy(
            slots_hbm.at[0, :, :, columns_of(order[step] * pair + core)],
            mine.at[step],
            slot_sems.at[1, step],
        )
        for step in range(chips)
    ]

    barrier = pltpu.get_barrier_semaphore()
    for side in (0, 1):
        @pl.when(has_row[side])
        def _():
            pl.semaphore_signal(barrier, inc=1, device_id=row_device[side], device_id_type=MESH)
    for by in range(1, group):
        pl.semaphore_signal(
            barrier, inc=1, device_id=(w, lax.rem(n + by, group)), device_id_type=MESH
        )
    for load in give_loads[:1] + mine_loads[:1] + small + give_loads[1:] + mine_loads[1:]:
        load.start()

    halo_rows = (slice(0, ROWS), slice(ROWS + height, extended))
    zeros = jnp.zeros((ROWS, width), jnp.float32)
    for side in (0, 1):
        @pl.when(jnp.logical_not(has_row[side]))
        def _():
            for i in range(3):
                fixed[i, halo_rows[side], :] = zeros
            given[layers, halo_rows[side], :] = zeros
            inner = slice(ROWS + halo_rows[side].start, ROWS + halo_rows[side].stop)
            for k in range(layers):
                field[0, k, inner, :] = zeros
                grad[STEPS - 1, k, inner, :] = zeros

        @pl.when(jnp.logical_not(has_col[side]))
        def _():
            for i in range(3):
                fixed_col[side, i] = jnp.zeros((height, LANES), jnp.float32)
            for i in range(layers + 1):
                given_col[side, i] = jnp.zeros((height, LANES), jnp.float32)
            for k in range(layers):
                field_col[side, k] = jnp.zeros((height, LANES), jnp.float32)

    for past in (slice(0, ROWS), slice(extended + ROWS, extended + 2 * ROWS)):
        for step in range(STEPS):
            for k in range(layers):
                field[step, k, past, :] = zeros
                grad[step, k, past, :] = zeros
        for t in range(4):
            wr[t, past, :] = zeros

    small[3].wait()
    for r in range(0, height, ROWS):
        fixed[2, ROWS + r : 2 * ROWS + r, 0:breadth] = sea_ref[r : r + ROWS, :].astype(jnp.float32)
    small[4].wait()
    small[5].wait()

    arrivals = group - 1 + has_row[0].astype(jnp.int32) + has_row[1].astype(jnp.int32)
    pl.semaphore_wait(barrier, arrivals)

    def near_copy(step, i):
        return remote(
            give.at[step, :, parts[i], :],
            near.at[step, :, parts[i], :],
            near_sems.at[0, step, i],
            near_sems.at[1, step, i],
            partner,
        )

    def far_copy(step, name):
        kind, a, b = name
        if kind == "edge":
            spot = (slice(None), parts[a], edge[b])
        elif kind == "inner":
            spot = (a, parts[b], slice(LANES, breadth - LANES))
        else:
            spot = (slice(None), parts[2], slice(LANES, breadth - LANES))
        at = far_names.index(name)
        return remote(
            mixed.at[(step, *spot)],
            far.at[(step, *spot)],
            far_sems.at[0, step, at],
            far_sems.at[1, step, at],
            (w, order[step] * pair + core),
        )

    far_names = (
        [("edge", i, side) for i in (0, 1) for side in (0, 1)]
        + [("inner", k, i) for k in range(layers) for i in (0, 1)]
        + [("edge", 2, side) for side in (0, 1)]
        + [("middle", 0, 0)]
    )

    give_loads[0].wait()
    for step in range(chips):
        if step:
            give_loads[step].wait()
        for i in range(3):
            near_copy(step, i).start()

    def fixed_row(side):
        source = halo_rows[side].start + (ROWS if side == 0 else -ROWS)
        return remote(
            fixed.at[:, source : source + ROWS, 0:breadth],
            fixed.at[:, halo_rows[1 - side], 0:breadth],
            fixed_sems.at[0, 0, side],
            fixed_sems.at[1, 0, 1 - side],
            row_device[side],
        )

    def fixed_column(side):
        return remote(
            fixed.at[:, own, edge[side]],
            fixed_col.at[1 - side],
            fixed_sems.at[0, 1, side],
            fixed_sems.at[1, 1, 1 - side],
            col_device[side],
        )

    def fixed_corner(side):
        source = halo_rows[side].start + (ROWS if side == 0 else -ROWS)
        return remote(
            fixed.at[:, source : source + ROWS, side_block],
            fixed.at[:, halo_rows[1 - side], side_block],
            fixed_sems.at[0, 2, side],
            fixed_sems.at[1, 2, 1 - side],
            row_device[side],
        )

    def given_column(side):
        return remote(
            given.at[:, own, edge[side]],
            given_col.at[1 - side],
            given_sems.at[0, 0, side],
            given_sems.at[1, 0, 1 - side],
            col_device[side],
        )

    def given_row(side):
        source = halo_rows[side].start + (ROWS if side == 0 else -ROWS)
        return remote(
            given.at[layers, source : source + ROWS, :],
            given.at[layers, halo_rows[1 - side], :],
            given_sems.at[0, 1, side],
            given_sems.at[1, 1, 1 - side],
            row_device[side],
        )

    def start(has, *makers):
        for side in (0, 1):
            @pl.when(has[side])
            def _():
                for maker in makers:
                    maker(side).start()

    def arrived(has, *makers):
        for side in (0, 1):
            @pl.when(has[side])
            def _():
                for maker in makers:
                    maker(1 - side).wait_recv()

    start(has_col, fixed_column)
    start(has_row, fixed_row)

    small[0].wait()

    def mix(step, k, rows, lanes):
        mixed[step, k, rows, lanes] = jnp.where(
            owner_ref[k] == n, mine[step, k, rows, lanes], near[step, k, rows, lanes]
        )

    def blocks_of(rows):
        return [slice(r, r + ROWS) for r in range(rows.start, rows.stop, ROWS)]

    everything = slice(0, breadth)
    for step in range(chips - 1):
        mine_loads[step].wait()
        for i in (0, 1):
            near_copy(step, i).wait_recv()
            for k in range(layers):
                mix(step, k, parts[i], everything)
            for side in (0, 1):
                far_copy(step, ("edge", i, side)).start()
        for k in range(layers):
            for i in (0, 1):
                far_copy(step, ("inner", k, i)).start()
        near_copy(step, 2).wait_recv()
        for k in range(layers):
            for rows in blocks_of(parts[2]):
                mix(step, k, rows, everything)
        for side in (0, 1):
            far_copy(step, ("edge", 2, side)).start()
        far_copy(step, ("middle", 0, 0)).start()

    last = chips - 1
    mine_loads[last].wait()
    for i in range(3):
        near_copy(last, i).wait_recv()

    small[1].wait()
    small[2].wait()
    speeds = []
    for k in range(layers):
        total = 0.0
        for c in range(speed_ref.shape[0]):
            total = jnp.where(class_ref[k] == c, speed_ref[c], total)
        speeds.append(total)

    def join(right, left):
        lane = lax.broadcasted_iota(jnp.int32, right.shape, right.ndim - 1)
        return jnp.where(lane < LANES // 2, right, left)

    arrived(has_col, fixed_column)
    for i in range(3):
        for r in range(0, height, ROWS):
            rows = slice(r, r + ROWS)
            fixed[i, ROWS + r : 2 * ROWS + r, side_block] = join(
                fixed_col[1, i, rows, :], fixed_col[0, i, rows, :]
            )
    start(has_row, fixed_corner)

    def make_weights(b):
        rows = slice(b * ROWS, (b + 1) * ROWS)
        inner = slice((b + 1) * ROWS, (b + 2) * ROWS)
        row_w = stencil_weights(fixed[0, rows, :])
        col_w = stencil_weights(fixed[1, rows, :])
        for t, offset in enumerate(OFFSETS):
            wr[t, inner, :] = row_w[offset + 2]
            wc[t, rows, :] = col_w[offset + 2]
            wc_back[3 - t, rows, :] = pltpu.roll(col_w[offset + 2], offset % width, 1)
        centre[rows, :] = 1.0 + row_w[2] + col_w[2]

    def turn_weights(b):
        for t, offset in enumerate(OFFSETS):
            base = (b + 1) * ROWS + offset
            wr_back[t, b * ROWS : (b + 1) * ROWS, :] = wr[3 - t, base : base + ROWS, :]

    for b in all_blocks[1:-1]:
        make_weights(b)

    small[6].wait()
    small[7].wait()
    start(has_col, given_column)

    def chosen(k, rows, lanes):
        value = jnp.where(
            owner_ref[k] == n, mine[last, k, rows, lanes], near[last, k, rows, lanes]
        )
        for step in range(chips - 1):
            sender = lax.rem(chip + chips - 1 - step, chips)
            value = jnp.where(
                lax.div(owner_ref[k], pair) == sender, far[step, k, rows, lanes], value
            )
        return value

    def put(k, rows, lanes):
        for piece in blocks_of(rows):
            spot = slice(2 * ROWS + piece.start, 2 * ROWS + piece.stop)
            field[0, k, spot, lanes] = chosen(k, piece, lanes)

    def shifted(rows):
        return slice(2 * ROWS + rows.start, 2 * ROWS + rows.stop)

    def field_column(i):
        def make(side):
            return remote(
                field.at[0, :, shifted(parts[i]), edge[side]],
                field_col.at[1 - side, :, parts[i], :],
                col_sems.at[0, i, side],
                col_sems.at[1, i, 1 - side],
                col_device[side],
            )

        return make

    wide_halo = (slice(ROWS, 2 * ROWS), slice(2 * ROWS + height, 3 * ROWS + height))

    def field_row(k):
        def make(side):
            return remote(
                field.at[0, k, shifted(parts[side]), 0:breadth],
                field.at[0, k, wide_halo[1 - side], 0:breadth],
                row_sems.at[0, k, side],
                row_sems.at[1, k, 1 - side],
                row_device[side],
            )

        return make

    def field_corner(side):
        return remote(
            field.at[0, :, shifted(parts[side]), side_block],
            field.at[0, :, wide_halo[1 - side], side_block],
            corner_sems.at[0, side],
            corner_sems.at[1, 1 - side],
            row_device[side],
        )

    def take(name):
        for step in range(chips - 1):
            far_copy(step, name).wait_recv()

    for i in (0, 1):
        for side in (0, 1):
            take(("edge", i, side))
            for k in range(layers):
                put(k, parts[i], edge[side])
        start(has_col, field_column(i))
    for k in range(layers):
        for i in (0, 1):
            take(("inner", k, i))
            put(k, parts[i], slice(LANES, breadth - LANES))

            @pl.when(has_row[i])
            def _():
                field_row(k)(i).start()
    for side in (0, 1):
        take(("edge", 2, side))
        for k in range(layers):
            put(k, parts[2], edge[side])
    start(has_col, field_column(2))

    def join_field(rows):
        for k in range(layers):
            for piece in blocks_of(rows):
                field[0, k, shifted(piece), side_block] = join(
                    field_col[1, k, piece, :], field_col[0, k, piece, :]
                )

    for i in (0, 1):
        arrived(has_col, field_column(i))
        join_field(parts[i])

        @pl.when(has_row[i])
        def _():
            field_corner(i).start()

    arrived(has_col, given_column)
    for i in range(layers + 1):
        for r in range(0, height, ROWS):
            rows = slice(r, r + ROWS)
            given[i, ROWS + r : 2 * ROWS + r, side_block] = join(
                given_col[1, i, rows, :], given_col[0, i, rows, :]
            )
    start(has_row, given_row)

    take(("middle", 0, 0))
    for k in range(layers):
        put(k, parts[2], slice(LANES, breadth - LANES))

    arrived(has_row, fixed_row, fixed_corner)
    make_weights(0)
    make_weights(all_blocks[-1])
    for b in all_blocks:
        turn_weights(b)

    arrived(has_col, field_column(2))
    join_field(parts[2])
    arrived(has_row, *[field_row(k) for k in range(layers)], field_corner)

    def stencil(source, b, rows_w, cols_w):
        base = (b + 1) * ROWS
        rows = slice(b * ROWS, (b + 1) * ROWS)
        here = source[base : base + ROWS, :]
        total = centre[rows, :] * here
        for t, o in enumerate(OFFSETS):
            total += rows_w[t] * source[base + o : base + o + ROWS, :]
            total += cols_w[t] * pltpu.roll(here, (-o) % width, 1)
        return total

    def forward(step, b):
        rows = slice(b * ROWS, (b + 1) * ROWS)
        inner = slice((b + 1) * ROWS, (b + 2) * ROWS)
        rows_w = [wr[t, inner, :] for t in range(4)]
        cols_w = [wc[t, rows, :] for t in range(4)]
        above = None
        for k in range(layers):
            adv = stencil(field.at[step, k], b, rows_w, cols_w)
            square = adv * adv
            part = 1.0 / (1.0 + square)
            slope[step, k, rows, :] = speeds[k] * (1.0 - square) * part * part
            if step + 1 < STEPS:
                flux = speeds[k] * adv * part
                left = adv - flux
                if above is not None:
                    left = left + above
                field[step + 1, k, inner, :] = left * fixed[2, rows, :]
                above = flux

    def settle_back(step, b, adjoint):
        rows = slice(b * ROWS, (b + 1) * ROWS)
        inner = slice((b + 1) * ROWS, (b + 2) * ROWS)
        mask = fixed[2, rows, :]
        below = mask * given[layers, rows, :]
        for k in reversed(range(layers)):
            masked = adjoint[k] * mask
            grad[step, k, inner, :] = masked + (below - masked) * slope[step, k, rows, :]
            below = masked

    def back(step, b):
        rows = slice(b * ROWS, (b + 1) * ROWS)
        rows_w = [wr_back[t, rows, :] for t in range(4)]
        cols_w = [wc_back[t, rows, :] for t in range(4)]
        adjoint = [stencil(grad.at[step, k], b, rows_w, cols_w) for k in range(layers)]
        if step:
            settle_back(step - 1, b, adjoint)
        else:
            spot = slice((b - 1) * ROWS, b * ROWS)
            for k in range(layers):
                out_ref[k, spot, :] = adjoint[k][:, 0:breadth]

    final_step = STEPS - 1

    def last_forward(b):
        forward(final_step, b)
        rows = slice(b * ROWS, (b + 1) * ROWS)
        settle_back(final_step, b, [given[k, rows, :] for k in range(layers)])

    quad = round_send.shape[2]

    def pieces():
        for k in range(layers):
            r = 0
            while r < REACH:
                at = k * REACH + r
                count = min(REACH - r, quad - at % quad)
                yield k, r, count, at // quad, at % quad
                r += count

    def round_copy(side):
        return remote(
            round_send.at[side],
            round_recv.at[1 - side],
            round_sems.at[0, side],
            round_sems.at[1, 1 - side],
            row_device[side],
        )

    def send_round(side):
        first = 2 * ROWS if side == 0 else 2 * ROWS + height - REACH
        for k, r, count, j, at in pieces():
            round_send[side, j, at : at + count, :] = grad[
                final_step, k, first + r : first + r + count, :
            ]

        @pl.when(has_row[side])
        def _():
            round_copy(side).start()

    def receive_round(side):
        first = 2 * ROWS - REACH if side == 0 else 2 * ROWS + height

        @pl.when(has_row[side])
        def _():
            round_copy(1 - side).wait_recv()
            for k, r, count, j, at in pieces():
                grad[final_step, k, first + r : first + r + count, :] = round_recv[
                    side, j, at : at + count, :
                ]

    for step in range(final_step):
        for b in all_blocks:
            forward(step, b)
    last_forward(1)
    send_round(0)
    last_forward(own_blocks)
    send_round(1)
    inside = all_blocks[2:-2]
    for b in inside:
        last_forward(b)

    for step in range(final_step, 0, -1):
        for b in all_blocks[1:-1]:
            back(step, b)
    for b in inside:
        back(0, b)

    arrived(has_row, given_row)
    outside = (all_blocks[:2], all_blocks[-2:])
    for side in (0, 1):
        receive_round(side)
        for step in range(final_step, 0, -1):
            for b in outside[side]:
                back(step, b)
    back(0, 1)
    back(0, own_blocks)

    def left(has, *makers):
        for side in (0, 1):
            @pl.when(has[side])
            def _():
                for maker in makers:
                    maker(side).wait_send()

    for step in range(chips):
        for i in range(3):
            near_copy(step, i).wait_send()
    for step in range(chips - 1):
        for name in far_names:
            far_copy(step, name).wait_send()
    left(has_col, fixed_column, given_column, *[field_column(i) for i in range(3)])
    left(
        has_row,
        fixed_row,
        fixed_corner,
        given_row,
        *[field_row(k) for k in range(layers)],
        field_corner,
        round_copy,
    )


def body(group_wide, group, slots, owner, row_v, col_v, land_sea, layer_class, speed, final, deposit):
    layers, height, breadth = final.shape
    chips = group // 2
    hops = max(chips - 1, 1)
    f32 = jnp.float32
    extended = height + 2 * ROWS
    padded = extended + 2 * ROWS
    width = breadth + LANES
    quads = layers * REACH // 4
    dma = pltpu.SemaphoreType.DMA
    vmem = pl.BlockSpec(memory_space=pltpu.VMEM)
    hbm = pl.BlockSpec(memory_space=pltpu.HBM)
    return pl.pallas_call(
        functools.partial(kernel, group_wide, group),
        out_shape=pltpu.VMEM(final.shape, f32),
        in_specs=[hbm] * 9,
        out_specs=vmem,
        scratch_shapes=[
            pltpu.SMEM(owner.shape, owner.dtype),
            pltpu.SMEM(layer_class.shape, layer_class.dtype),
            pltpu.SMEM(speed.shape, speed.dtype),
            pltpu.VMEM(land_sea.shape, land_sea.dtype),
            pltpu.VMEM((3, extended, width), f32),
            pltpu.VMEM((2, 3, height, LANES), f32),
            pltpu.VMEM((layers + 1, extended, width), f32),
            pltpu.VMEM((2, layers + 1, height, LANES), f32),
            pltpu.VMEM((chips, layers, height, breadth), f32),
            pltpu.VMEM((chips, layers, height, breadth), f32),
            pltpu.VMEM((chips, layers, height, breadth), f32),
            pltpu.VMEM((hops, layers, height, breadth), f32),
            pltpu.VMEM((hops, layers, height, breadth), f32),
            pltpu.VMEM((STEPS, layers, padded, width), f32),
            pltpu.VMEM((2, layers, height, LANES), f32),
            pltpu.VMEM((STEPS, layers, extended, width), f32),
            pltpu.VMEM((STEPS, layers, padded, width), f32),
            pltpu.VMEM((4, padded, width), f32),
            pltpu.VMEM((4, extended, width), f32),
            pltpu.VMEM((4, extended, width), f32),
            pltpu.VMEM((4, extended, width), f32),
            pltpu.VMEM((extended, width), f32),
            pltpu.VMEM((2, quads, 4, width), f32),
            pltpu.VMEM((2, quads, 4, width), f32),
            dma((8,)),
            dma((2, chips)),
            dma((2, chips, 3)),
            dma((2, hops, 7 + 2 * layers)),
            dma((2, 3, 2)),
            dma((2, 2, 2)),
            dma((2, 3, 2)),
            dma((2, layers, 2)),
            dma((2, 2)),
            dma((2, 2)),
        ],
        compiler_params=pltpu.CompilerParams(
            collective_id=0,
            has_side_effects=True,
            vmem_limit_bytes=VMEM_BYTES - final.size * final.dtype.itemsize,
        ),
    )(owner, layer_class, speed, slots, row_v, col_v, land_sea, final, deposit)


def solution(mesh):
    in_specs = (
        P("narrow", None, "wide", None),
        P(),
        P("wide", "narrow"),
        P("wide", "narrow"),
        P("wide", "narrow"),
        P(),
        P(),
        P(None, "wide", "narrow"),
        P("wide", "narrow"),
    )
    out_specs = P(None, "wide", "narrow")
    return jax.shard_map(
        functools.partial(body, mesh.shape["wide"], mesh.shape["narrow"]),
        mesh=mesh,
        in_specs=in_specs,
        out_specs=out_specs,
        check_vma=False,
    )
```

```python
import functools

import jax
import jax.numpy as jnp
from jax import lax
from jax.experimental import pallas as pl
from jax.experimental.pallas import tpu as pltpu
from jax.sharding import PartitionSpec as P

STEPS = 3
LANES = 128
ROWS = 8
HALF = ROWS // 2
SHARE = 16
OFFSETS = (-2, -1, 1, 2)
MESH = pl.DeviceIdType.MESH
VMEM_BYTES = 67043328


def stencil_weights(velocity):
    p = jnp.maximum(velocity, 0.0)
    q = jnp.minimum(velocity, 0.0)
    pp = p * p
    qq = q * q
    return [
        0.5 * pp - 0.5 * p,
        2.0 * p - pp,
        0.5 * pp - 1.5 * p + 0.5 * qq + 1.5 * q,
        -2.0 * q - qq,
        0.5 * qq + 0.5 * q,
    ]


def kernel(
    group_wide,
    group,
    owner_hbm,
    class_hbm,
    speed_hbm,
    slots_hbm,
    row_velocity_hbm,
    column_velocity_hbm,
    sea_hbm,
    final_hbm,
    deposit_hbm,
    out_ref,
    owner_ref,
    class_ref,
    speed_ref,
    sea_ref,
    fixed,
    fixed_inner,
    given,
    given_inner,
    outer_send,
    outer_recv,
    mine,
    give,
    near,
    mixed,
    far,
    field,
    field_inner,
    field_outer,
    field_late,
    slope,
    grad,
    wr,
    wc,
    wr_back,
    wc_back,
    centre,
    round_send,
    round_recv,
    load_sems,
    slot_sems,
    near_sems,
    far_sems,
    fixed_sems,
    given_sems,
    col_sems,
    row_sems,
    corner_sems,
    late_sems,
    round_sems,
):
    layers, height, breadth = out_ref.shape
    pair = 2
    chips = group // pair
    w = lax.axis_index("wide")
    n = lax.axis_index("narrow")
    chip = lax.div(n, pair)
    core = lax.rem(n, pair)
    width = breadth + LANES
    own_blocks = height // ROWS
    extended = height + 2 * ROWS
    all_blocks = list(range(own_blocks + 2))
    inside = all_blocks[2:-2]
    edge = (slice(0, LANES), slice(breadth - LANES, breadth))
    side_block = slice(breadth, width)
    own = slice(ROWS, ROWS + height)

    has_row = (w > 0, w < group_wide - 1)
    row_device = ((w - 1, n), (w + 1, n))
    partner = (w, chip * pair + (pair - 1 - core))
    order = [lax.rem(chip + by, chips) for by in range(1, chips)] + [chip]
    parts = (
        slice(0, ROWS),
        slice(height - ROWS, height),
        slice(ROWS, height - ROWS),
    )
    def pieces_at(first, last):
        return (slice(first, last), slice(height - last, height - first))

    rim = pieces_at(0, HALF)
    second = pieces_at(HALF, 2 * HALF)
    third = pieces_at(2 * HALF, 3 * HALF)
    inward = pieces_at(HALF, 3 * HALF)
    core_rows = slice(3 * HALF, height - 3 * HALF)

    def columns_of(device):
        return pl.ds(pl.multiple_of(device * breadth, LANES), breadth)

    def outer_columns(device, at_core):
        start = device * breadth - LANES + at_core * (breadth + LANES)
        return pl.ds(pl.multiple_of(lax.rem(start + group * breadth, group * breadth), LANES), LANES)

    def has_outer(device):
        beside = device - 1 + 2 * core
        return jnp.logical_and(beside >= 0, beside < group)

    def remote(src, dst, send_sem, recv_sem, device):
        return pltpu.make_async_remote_copy(
            src_ref=src,
            dst_ref=dst,
            send_sem=send_sem,
            recv_sem=recv_sem,
            device_id=device,
            device_id_type=MESH,
        )

    small = [
        pltpu.make_async_copy(source, target, load_sems.at[i])
        for i, (source, target) in enumerate(
            [
                (owner_hbm, owner_ref),
                (class_hbm, class_ref),
                (speed_hbm, speed_ref),
                (sea_hbm, sea_ref),
                (row_velocity_hbm, fixed.at[0, own, 0:breadth]),
                (column_velocity_hbm, fixed.at[1, own, 0:breadth]),
                (final_hbm, given.at[0:layers, own, 0:breadth]),
                (deposit_hbm, given.at[layers, own, 0:breadth]),
            ]
        )
    ]
    def slot_loads(target, row, at_core):
        return [
            [
                pltpu.make_async_copy(
                    slots_hbm.at[0, :, :, columns(order[step] * pair + at_core)],
                    target.at[step, :, :, lanes],
                    slot_sems.at[row, i, step],
                )
                for i, (columns, lanes) in enumerate(
                    [
                        (columns_of, slice(0, breadth)),
                        (functools.partial(outer_columns, at_core=at_core), side_block),
                    ]
                )
            ]
            for step in range(chips)
        ]

    give_loads = slot_loads(give, 0, pair - 1 - core)
    mine_loads = slot_loads(mine, 1, core)

    halo_rows = (slice(0, ROWS), slice(ROWS + height, extended))
    barrier = pltpu.get_barrier_semaphore()
    for side in (0, 1):
        @pl.when(has_row[side])
        def _():
            pl.semaphore_signal(barrier, inc=1, device_id=row_device[side], device_id_type=MESH)
    for by in range(1, group):
        pl.semaphore_signal(
            barrier, inc=1, device_id=(w, lax.rem(n + by, group)), device_id_type=MESH
        )
    for load in give_loads[0] + mine_loads[0] + small + sum(give_loads[1:] + mine_loads[1:], []):
        load.start()

    arrivals = group - 1 + has_row[0].astype(jnp.int32) + has_row[1].astype(jnp.int32)
    pl.semaphore_wait(barrier, arrivals)

    def near_copy(step, i):
        return remote(
            give.at[step, :, parts[i], :],
            near.at[step, :, parts[i], :],
            near_sems.at[step, 3],
            near_sems.at[step, i],
            partner,
        )

    def far_copy(step, name):
        kind, rows, side = name
        if kind == "edge":
            lanes = edge[side]
        elif kind == "outer":
            lanes = side_block
        else:
            lanes = slice(LANES, breadth - LANES)
        spot = (slice(None), rows, lanes)
        at = far_names.index(name)
        return remote(
            mixed.at[(step, *spot)],
            far.at[(step, *spot)],
            far_sems.at[step, len(far_names) + int(kind == "outer")],
            far_sems.at[step, at],
            (w, order[step] * pair + core),
        )

    def rims_of(rows):
        return [("edge", rows, 0), ("edge", rows, 1), ("outer", rows, 0)]

    def main_of(rows):
        return ("main", rows, 0)

    far_names = []
    for i in (0, 1):
        far_names += rims_of(rim[i])
    far_names += [main_of(rim[i]) for i in (0, 1)]
    early = len(far_names)
    for i in (0, 1):
        far_names += rims_of(inward[i])
    far_names += [main_of(second[i]) for i in (0, 1)]
    far_names += rims_of(core_rows)
    far_names += [main_of(third[i]) for i in (0, 1)]
    far_names += [main_of(core_rows)]

    def far_start(step, name):
        if name[0] == "outer":
            pl.when(has_outer(order[step] * pair + core))(far_copy(step, name).start)
        else:
            far_copy(step, name).start()

    for step in range(chips):
        for load in give_loads[step]:
            load.wait()
        for i in range(3):
            near_copy(step, i).start()

    inner_edge = pl.ds(pl.multiple_of((1 - core) * (breadth - LANES), LANES), LANES)
    outer_edge = pl.ds(pl.multiple_of(core * (breadth - LANES), LANES), LANES)
    def near_edge(side, first, last):
        if side == 0:
            return slice(ROWS + first, ROWS + last), slice(
                ROWS + height + first, ROWS + height + last
            )
        return slice(ROWS + height - last, ROWS + height - first), slice(ROWS - last, ROWS - first)

    def fixed_row(side):
        source, target = near_edge(side, 0, ROWS - 2)
        return remote(
            fixed.at[:, source, 0:breadth],
            fixed.at[:, target, 0:breadth],
            fixed_sems.at[0, 0, side],
            fixed_sems.at[1, 0, 1 - side],
            row_device[side],
        )

    def fixed_column():
        return remote(
            fixed.at[:, own, inner_edge],
            fixed_inner,
            fixed_sems.at[0, 1, 0],
            fixed_sems.at[1, 1, 0],
            partner,
        )

    def given_column():
        return remote(
            given.at[:, own, inner_edge],
            given_inner,
            given_sems.at[0, 0, 0],
            given_sems.at[1, 0, 0],
            partner,
        )

    def outer_column():
        return remote(
            outer_send,
            outer_recv,
            fixed_sems.at[0, 1, 1],
            fixed_sems.at[1, 1, 1],
            (w, n - 1 + 2 * core),
        )

    def fixed_corner(side):
        source, target = near_edge(side, 0, ROWS - 2)
        return remote(
            fixed.at[:, source, side_block],
            fixed.at[:, target, side_block],
            fixed_sems.at[0, 2, side],
            fixed_sems.at[1, 2, 1 - side],
            row_device[side],
        )

    def given_row(side):
        source, target = near_edge(side, 0, 2 * (STEPS - 1))
        return remote(
            given.at[layers, source, :],
            given.at[layers, target, :],
            given_sems.at[0, 1, side],
            given_sems.at[1, 1, 1 - side],
            row_device[side],
        )

    def final_row(side):
        source, target = near_edge(side, 0, 2)
        return remote(
            given.at[0:layers, source, :],
            given.at[0:layers, target, :],
            given_sems.at[0, 2, side],
            given_sems.at[1, 2, 1 - side],
            row_device[side],
        )

    def start(has, *makers):
        for side in (0, 1):
            @pl.when(has[side])
            def _():
                for maker in makers:
                    maker(side).start()

    def arrived(has, *makers):
        for side in (0, 1):
            @pl.when(has[side])
            def _():
                for maker in makers:
                    maker(1 - side).wait_recv()

    small[3].wait()
    for r in range(0, height, ROWS):
        fixed[2, ROWS + r : 2 * ROWS + r, 0:breadth] = sea_ref[r : r + ROWS, :].astype(jnp.float32)
    small[4].wait()
    small[5].wait()

    start(has_row, fixed_row)
    fixed_column().start()
    small[6].wait()
    small[7].wait()
    given_column().start()
    shared = [(fixed, i) for i in range(3)] + [(given, i) for i in range(layers + 1)]
    lane = lax.broadcasted_iota(jnp.int32, (ROWS, LANES), 1)
    for r in range(0, height, ROWS):
        packed = jnp.zeros((ROWS, LANES), jnp.float32)
        for a, (ref, i) in enumerate(shared):
            moved = pltpu.roll(ref[i, ROWS + r : 2 * ROWS + r, outer_edge], SHARE * (a + core), 1)
            mine_lanes = jnp.logical_and(lane >= SHARE * a, lane < SHARE * (a + 1))
            packed = jnp.where(mine_lanes, moved, packed)
        outer_send[r : r + ROWS, :] = packed
    pl.when(has_outer(n))(outer_column().start)

    small[0].wait()

    def mix(step, k, rows, lanes):
        mixed[step, k, rows, lanes] = jnp.where(
            owner_ref[k] == n, mine[step, k, rows, lanes], near[step, k, rows, lanes]
        )

    def blocks_of(rows):
        return [slice(r, r + ROWS) for r in range(rows.start, rows.stop, ROWS)]

    everything = slice(0, width)
    for step in range(chips - 1):
        for load in mine_loads[step]:
            load.wait()
        for i in range(3):
            near_copy(step, i).wait_recv()
            for k in range(layers):
                for rows in blocks_of(parts[i]):
                    mix(step, k, rows, everything)
            if i == 1:
                for name in far_names[:early]:
                    far_start(step, name)
            elif i == 2:
                for name in far_names[early:]:
                    far_start(step, name)

    zeros = jnp.zeros((ROWS, width), jnp.float32)
    for side in (0, 1):
        @pl.when(jnp.logical_not(has_row[side]))
        def _():
            for i in range(3):
                fixed[i, halo_rows[side], :] = zeros
            for i in range(layers + 1):
                given[i, halo_rows[side], :] = zeros
            inner = slice(ROWS + halo_rows[side].start, ROWS + halo_rows[side].stop)
            for k in range(layers):
                field[0, k, inner, :] = zeros
                grad[STEPS - 1, k, inner, :] = zeros

    for past in (slice(0, ROWS), slice(extended + ROWS, extended + 2 * ROWS)):
        for step in range(STEPS):
            for k in range(layers):
                field[step, k, past, :] = zeros
                grad[step, k, past, :] = zeros
        for t in range(4):
            wr[t, past, :] = zeros

    last = chips - 1
    for load in mine_loads[last]:
        load.wait()
    for i in range(3):
        near_copy(last, i).wait_recv()

    small[1].wait()
    small[2].wait()
    speeds = []
    for k in range(layers):
        total = 0.0
        for c in range(speed_ref.shape[0]):
            total = jnp.where(class_ref[k] == c, speed_ref[c], total)
        speeds.append(total)

    upper = (lane >= LANES // 2).astype(jnp.int32)
    fixed_column().wait_recv()
    given_column().wait_recv()
    pl.when(has_outer(n))(outer_column().wait_recv)
    for a, (ref, i) in enumerate(shared):
        inner_ref = (fixed_inner, given_inner)[a >= 3]
        for r in range(0, height, ROWS):
            rows = slice(r, r + ROWS)
            back_by = lax.rem(2 * LANES - SHARE * (a + 1 - core), LANES)
            outer = jnp.where(has_outer(n), pltpu.roll(outer_recv[rows, :], back_by, 1), 0.0)
            ref[i, ROWS + r : 2 * ROWS + r, side_block] = jnp.where(
                upper == core, inner_ref[i, rows, :], outer
            )
    start(has_row, fixed_corner, final_row, given_row)

    def make_weights(b):
        rows = slice(b * ROWS, (b + 1) * ROWS)
        inner = slice((b + 1) * ROWS, (b + 2) * ROWS)
        row_w = stencil_weights(fixed[0, rows, :])
        col_w = stencil_weights(fixed[1, rows, :])
        for t, offset in enumerate(OFFSETS):
            wr[t, inner, :] = row_w[offset + 2]
            wc[t, rows, :] = col_w[offset + 2]
            wc_back[3 - t, rows, :] = pltpu.roll(col_w[offset + 2], offset % width, 1)
        centre[rows, :] = 1.0 + row_w[2] + col_w[2]

    def turn_weights(b):
        for t, offset in enumerate(OFFSETS):
            base = (b + 1) * ROWS + offset
            wr_back[t, b * ROWS : (b + 1) * ROWS, :] = wr[3 - t, base : base + ROWS, :]

    for b in all_blocks[1:-1]:
        make_weights(b)

    for b in inside:
        turn_weights(b)

    def chosen(k, rows, lanes):
        value = jnp.where(
            owner_ref[k] == n, mine[last, k, rows, lanes], near[last, k, rows, lanes]
        )
        for step in range(chips - 1):
            sender = lax.rem(chip + chips - 1 - step, chips)
            value = jnp.where(
                lax.div(owner_ref[k], pair) == sender, far[step, k, rows, lanes], value
            )
        return value

    def put(rows, lanes):
        for k in range(layers):
            for piece in halves_of(rows):
                field[0, k, shifted(piece), lanes] = chosen(k, piece, lanes)

    def halves_of(rows):
        return [slice(r, r + HALF) for r in range(rows.start, rows.stop, HALF)]

    def shifted(rows):
        return slice(2 * ROWS + rows.start, 2 * ROWS + rows.stop)

    swaps = [*rim, *inward, core_rows]

    def field_column(rows):
        at = swaps.index(rows)
        return remote(
            field.at[0, :, shifted(rows), inner_edge],
            field_inner.at[:, rows, :],
            col_sems.at[0, at],
            col_sems.at[1, at],
            partner,
        )

    halo_near = (
        slice(2 * ROWS - HALF, 2 * ROWS),
        slice(2 * ROWS + height, 2 * ROWS + height + HALF),
    )
    halo_beyond = (
        slice(ROWS, 2 * ROWS - HALF),
        slice(2 * ROWS + height + HALF, 3 * ROWS + height),
    )

    def field_row(side):
        return remote(
            field.at[0, :, shifted(rim[side]), 0:breadth],
            field.at[0, :, halo_near[1 - side], 0:breadth],
            row_sems.at[0, side],
            row_sems.at[1, 1 - side],
            row_device[side],
        )

    def field_corner(side):
        return remote(
            field.at[0, :, shifted(rim[side]), side_block],
            field.at[0, :, halo_near[1 - side], side_block],
            corner_sems.at[0, side],
            corner_sems.at[1, 1 - side],
            row_device[side],
        )

    def late_row(side):
        return remote(
            field.at[0, :, shifted(second[side]), :],
            field_late.at[1 - side],
            late_sems.at[0, side],
            late_sems.at[1, 1 - side],
            row_device[side],
        )

    def start_row(side, maker):
        pl.when(has_row[side])(maker(side).start)

    def take(name):
        for step in range(chips - 1):
            if name[0] == "outer":
                pl.when(has_outer(n))(far_copy(step, name).wait_recv)
            else:
                far_copy(step, name).wait_recv()

    def put_outer(rows):
        for k in range(layers):
            for piece in halves_of(rows):
                value = chosen(k, piece, side_block)
                field_outer[k, piece, :] = jnp.where(has_outer(n), value, 0.0)

    def join_field(rows):
        field_column(rows).wait_recv()
        for k in range(layers):
            for piece in halves_of(rows):
                field[0, k, shifted(piece), side_block] = jnp.where(
                    upper[:HALF] == core, field_inner[k, piece, :], field_outer[k, piece, :]
                )

    def take_rims(rows):
        for side in (0, 1):
            take(("edge", rows, side))
            put(rows, edge[side])
        field_column(rows).start()
        take(("outer", rows, 0))
        put_outer(rows)

    def take_main(rows):
        take(main_of(rows))
        put(rows, slice(LANES, breadth - LANES))

    for i in (0, 1):
        take_rims(rim[i])
    for i in (0, 1):
        take_main(rim[i])
        start_row(i, field_row)
        join_field(rim[i])
        start_row(i, field_corner)
    arrived(has_row, fixed_row, fixed_corner)
    make_weights(0)
    make_weights(all_blocks[-1])
    for i in (0, 1):
        take_rims(inward[i])
    for i in (0, 1):
        take_main(second[i])
        join_field(inward[i])
        start_row(i, late_row)
    take_rims(core_rows)
    for i in (0, 1):
        take_main(third[i])

    arrived(has_row, field_row, field_corner)

    def stencil(source, b, rows_w, cols_w):
        base = (b + 1) * ROWS
        rows = slice(b * ROWS, (b + 1) * ROWS)
        here = source[base : base + ROWS, :]
        total = centre[rows, :] * here
        for t, o in enumerate(OFFSETS):
            total += rows_w[t] * source[base + o : base + o + ROWS, :]
            total += cols_w[t] * pltpu.roll(here, (-o) % width, 1)
        return total

    def forward(step, b):
        rows = slice(b * ROWS, (b + 1) * ROWS)
        inner = slice((b + 1) * ROWS, (b + 2) * ROWS)
        rows_w = [wr[t, inner, :] for t in range(4)]
        cols_w = [wc[t, rows, :] for t in range(4)]
        above = None
        for k in range(layers):
            adv = stencil(field.at[step, k], b, rows_w, cols_w)
            square = adv * adv
            part = 1.0 / (1.0 + square)
            slope[step, k, rows, :] = speeds[k] * (1.0 - square) * part * part
            if step + 1 < STEPS:
                flux = speeds[k] * adv * part
                left = adv - flux
                if above is not None:
                    left = left + above
                field[step + 1, k, inner, :] = left * fixed[2, rows, :]
                above = flux

    def settle_back(step, b, adjoint, keep):
        rows = slice(b * ROWS, (b + 1) * ROWS)
        mask = fixed[2, rows, :]
        below = mask * given[layers, rows, :]
        for k in reversed(range(layers)):
            masked = adjoint[k] * mask
            keep(k, masked + (below - masked) * slope[step, k, rows, :])
            below = masked

    def keep_grad(step, b, first=0, last=ROWS):
        base = (b + 1) * ROWS

        def keep(k, value):
            grad[step, k, base + first : base + last, :] = value[first:last, :]

        return keep

    def back(step, b):
        rows = slice(b * ROWS, (b + 1) * ROWS)
        rows_w = [wr_back[t, rows, :] for t in range(4)]
        cols_w = [wc_back[t, rows, :] for t in range(4)]
        adjoint = [stencil(grad.at[step, k], b, rows_w, cols_w) for k in range(layers)]
        if step:
            settle_back(step - 1, b, adjoint, keep_grad(step - 1, b))
        else:
            spot = slice((b - 1) * ROWS, b * ROWS)
            for k in range(layers):
                out_ref[k, spot, :] = adjoint[k][:, 0:breadth]

    final_step = STEPS - 1

    def last_forward(b, keep):
        forward(final_step, b)
        rows = slice(b * ROWS, (b + 1) * ROWS)
        settle_back(final_step, b, [given[k, rows, :] for k in range(layers)], keep)

    def round_copy(side):
        return remote(
            round_send.at[side],
            round_recv.at[1 - side],
            round_sems.at[0, side],
            round_sems.at[1, 1 - side],
            row_device[side],
        )

    def receive_round(side):
        first = 2 * ROWS - 2 - HALF if side == 0 else 2 * ROWS + height + 2

        @pl.when(has_row[side])
        def _():
            round_copy(1 - side).wait_recv()
            for k in range(layers):
                grad[final_step, k, first : first + HALF, :] = round_recv[side, k]

    outside = (all_blocks[:2], all_blocks[-2:])
    for side in (0, 1):
        b = outside[side][1 - side]
        for at in (b - 1, b, b + 1):
            forward(0, at)
        for step in range(1, final_step):
            forward(step, b)
        first = 2 if side == 0 else ROWS - 2 - HALF

        def keep(k, value):
            round_send[side, k] = value[first : first + HALF, :]

        last_forward(b, keep)
        start_row(side, round_copy)

    take_main(core_rows)
    join_field(core_rows)
    for step in range(final_step):
        for b in inside:
            forward(step, b)
    for b in inside:
        last_forward(b, keep_grad(final_step, b))
    for side in (0, 1):
        @pl.when(has_row[side])
        def _():
            late_row(1 - side).wait_recv()
            for k in range(layers):
                field[0, k, halo_beyond[side], :] = field_late[side, k]

    ends = (all_blocks[0], all_blocks[-1])
    for step in range(final_step):
        for b in ends:
            forward(step, b)
    arrived(has_row, final_row, given_row)
    for side in (0, 1):
        b = outside[side][1 - side]
        last_forward(b, keep_grad(final_step, b))
        spot = (ROWS - 2, ROWS) if side == 0 else (0, 2)
        last_forward(ends[side], keep_grad(final_step, ends[side], *spot))
    for b in (*outside[0], *outside[1]):
        turn_weights(b)

    for step in range(final_step, 0, -1):
        for b in all_blocks[1:-1]:
            back(step, b)
    for b in inside:
        back(0, b)

    for side in (0, 1):
        receive_round(side)
        for step in range(final_step, 0, -1):
            for b in outside[side]:
                back(step, b)
    back(0, 1)
    back(0, own_blocks)

    def left(has, *makers):
        for side in (0, 1):
            @pl.when(has[side])
            def _():
                for maker in makers:
                    maker(side).wait_send()

    for step in range(chips):
        remote(give.at[step], near.at[step], near_sems.at[step, 3], near_sems.at[step, 0], partner).wait_send()
    for step in range(chips - 1):
        device = order[step] * pair + core
        for i, lanes in enumerate((slice(0, breadth), side_block)):
            sent = remote(
                mixed.at[step, :, :, lanes],
                far.at[step, :, :, lanes],
                far_sems.at[step, len(far_names) + i],
                far_sems.at[step, 0],
                (w, device),
            )
            if i == 0:
                sent.wait_send()
            else:
                pl.when(has_outer(device))(sent.wait_send)
    for rows in swaps:
        field_column(rows).wait_send()
    fixed_column().wait_send()
    given_column().wait_send()
    pl.when(has_outer(n))(outer_column().wait_send)
    left(
        has_row,
        fixed_row,
        fixed_corner,
        given_row,
        final_row,
        field_row,
        field_corner,
        late_row,
        round_copy,
    )


def body(group_wide, group, slots, owner, row_v, col_v, land_sea, layer_class, speed, final, deposit):
    layers, height, breadth = final.shape
    chips = group // 2
    hops = max(chips - 1, 1)
    f32 = jnp.float32
    extended = height + 2 * ROWS
    padded = extended + 2 * ROWS
    width = breadth + LANES
    dma = pltpu.SemaphoreType.DMA
    vmem = pl.BlockSpec(memory_space=pltpu.VMEM)
    hbm = pl.BlockSpec(memory_space=pltpu.HBM)
    return pl.pallas_call(
        functools.partial(kernel, group_wide, group),
        out_shape=pltpu.VMEM(final.shape, f32),
        in_specs=[hbm] * 9,
        out_specs=vmem,
        scratch_shapes=[
            pltpu.SMEM(owner.shape, owner.dtype),
            pltpu.SMEM(layer_class.shape, layer_class.dtype),
            pltpu.SMEM(speed.shape, speed.dtype),
            pltpu.VMEM(land_sea.shape, land_sea.dtype),
            pltpu.VMEM((3, extended, width), f32),
            pltpu.VMEM((3, height, LANES), f32),
            pltpu.VMEM((layers + 1, extended, width), f32),
            pltpu.VMEM((layers + 1, height, LANES), f32),
            pltpu.VMEM((height, LANES), f32),
            pltpu.VMEM((height, LANES), f32),
            pltpu.VMEM((chips, layers, height, width), f32),
            pltpu.VMEM((chips, layers, height, width), f32),
            pltpu.VMEM((chips, layers, height, width), f32),
            pltpu.VMEM((hops, layers, height, width), f32),
            pltpu.VMEM((hops, layers, height, width), f32),
            pltpu.VMEM((STEPS, layers, padded, width), f32),
            pltpu.VMEM((layers, height, LANES), f32),
            pltpu.VMEM((layers, height, LANES), f32),
            pltpu.VMEM((2, layers, HALF, width), f32),
            pltpu.VMEM((STEPS, layers, extended, width), f32),
            pltpu.VMEM((STEPS, layers, padded, width), f32),
            pltpu.VMEM((4, padded, width), f32),
            pltpu.VMEM((4, extended, width), f32),
            pltpu.VMEM((4, extended, width), f32),
            pltpu.VMEM((4, extended, width), f32),
            pltpu.VMEM((extended, width), f32),
            pltpu.VMEM((2, layers, HALF, width), f32),
            pltpu.VMEM((2, layers, HALF, width), f32),
            dma((8,)),
            dma((2, 2, chips)),
            dma((chips, 4)),
            dma((hops, 22 + 2)),
            dma((2, 3, 2)),
            dma((2, 3, 2)),
            dma((2, 5)),
            dma((2, 2)),
            dma((2, 2)),
            dma((2, 2)),
            dma((2, 2)),
        ],
        compiler_params=pltpu.CompilerParams(
            collective_id=0,
            has_side_effects=True,
            vmem_limit_bytes=VMEM_BYTES - final.size * final.dtype.itemsize,
        ),
    )(owner, layer_class, speed, slots, row_v, col_v, land_sea, final, deposit)


def solution(mesh):
    in_specs = (
        P("narrow", None, "wide", None),
        P(),
        P("wide", "narrow"),
        P("wide", "narrow"),
        P("wide", "narrow"),
        P(),
        P(),
        P(None, "wide", "narrow"),
        P("wide", "narrow"),
    )
    out_specs = P(None, "wide", "narrow")
    return jax.shard_map(
        functools.partial(body, mesh.shape["wide"], mesh.shape["narrow"]),
        mesh=mesh,
        in_specs=in_specs,
        out_specs=out_specs,
        check_vma=False,
    )
```

```python
import functools

import jax
import jax.numpy as jnp
from jax import lax
from jax.experimental import pallas as pl
from jax.experimental.pallas import tpu as pltpu
from jax.sharding import PartitionSpec as P

STEPS = 3
LANES = 128
ROWS = 8
HALF = ROWS // 2
SHARE = 16
CHUNK = 3
OFFSETS = (-2, -1, 1, 2)
MESH = pl.DeviceIdType.MESH
VMEM_BYTES = 67043328


def stencil_weights(velocity):
    p = jnp.maximum(velocity, 0.0)
    q = jnp.minimum(velocity, 0.0)
    pp = p * p
    qq = q * q
    return [
        0.5 * pp - 0.5 * p,
        2.0 * p - pp,
        0.5 * pp - 1.5 * p + 0.5 * qq + 1.5 * q,
        -2.0 * q - qq,
        0.5 * qq + 0.5 * q,
    ]


def kernel(
    group_wide,
    group,
    owner_hbm,
    class_hbm,
    speed_hbm,
    slots_hbm,
    row_velocity_hbm,
    column_velocity_hbm,
    sea_hbm,
    final_hbm,
    deposit_hbm,
    out_ref,
    owner_ref,
    class_ref,
    speed_ref,
    sea_ref,
    fixed,
    fixed_inner,
    given,
    given_inner,
    outer_send,
    outer_recv,
    mine,
    give,
    near,
    mixed,
    far,
    field,
    field_inner,
    field_outer,
    field_late,
    slope,
    grad,
    wr,
    wc,
    wr_back,
    wc_back,
    centre,
    sea,
    final_masked,
    deposit_masked,
    round_send,
    round_recv,
    load_sems,
    slot_sems,
    near_sems,
    far_sems,
    fixed_sems,
    given_sems,
    col_sems,
    row_sems,
    late_sems,
    round_sems,
):
    layers, height, breadth = out_ref.shape
    pair = 2
    chips = group // pair
    w = lax.axis_index("wide")
    n = lax.axis_index("narrow")
    chip = lax.div(n, pair)
    core = lax.rem(n, pair)
    width = breadth + LANES
    tiles = breadth // LANES
    own_blocks = height // ROWS
    extended = height + 2 * ROWS
    all_blocks = list(range(own_blocks + 2))
    inside = all_blocks[2:-2]
    edge = (slice(0, LANES), slice(breadth - LANES, breadth))
    side_block = slice(breadth, width)
    own = slice(ROWS, ROWS + height)

    has_row = (w > 0, w < group_wide - 1)
    row_device = ((w - 1, n), (w + 1, n))
    partner = (w, chip * pair + (pair - 1 - core))
    order = [lax.rem(chip + by, chips) for by in range(1, chips)] + [chip]
    parts = (
        slice(0, ROWS),
        slice(height - ROWS, height),
        slice(ROWS, height - ROWS),
    )
    def pieces_at(first, last):
        return (slice(first, last), slice(height - last, height - first))

    rim = pieces_at(0, HALF)
    second = pieces_at(HALF, 2 * HALF)
    third = pieces_at(2 * HALF, 3 * HALF)
    inward = pieces_at(HALF, 3 * HALF)
    core_rows = slice(3 * HALF, height - 3 * HALF)

    def columns_of(device):
        return pl.ds(pl.multiple_of(device * breadth, LANES), breadth)

    def outer_columns(device, at_core):
        start = device * breadth - LANES + at_core * (breadth + LANES)
        return pl.ds(pl.multiple_of(lax.rem(start + group * breadth, group * breadth), LANES), LANES)

    def has_outer(device):
        beside = device - 1 + 2 * core
        return jnp.logical_and(beside >= 0, beside < group)

    def remote(src, dst, send_sem, recv_sem, device):
        return pltpu.make_async_remote_copy(
            src_ref=src,
            dst_ref=dst,
            send_sem=send_sem,
            recv_sem=recv_sem,
            device_id=device,
            device_id_type=MESH,
        )

    small = [
        pltpu.make_async_copy(source, target, load_sems.at[(0, 1, 2, 3, 3, 3, 4, 4)[i]])
        for i, (source, target) in enumerate(
            [
                (owner_hbm, owner_ref),
                (class_hbm, class_ref),
                (speed_hbm, speed_ref),
                (sea_hbm, sea_ref),
                (row_velocity_hbm, fixed.at[0, own, 0:breadth]),
                (column_velocity_hbm, fixed.at[1, own, 0:breadth]),
                (final_hbm, given.at[0:layers, own, 0:breadth]),
                (deposit_hbm, given.at[layers, own, 0:breadth]),
            ]
        )
    ]
    def slot_loads(target, row, at_core):
        return [
            [
                pltpu.make_async_copy(
                    slots_hbm.at[0, :, :, columns(order[step] * pair + at_core)],
                    target.at[step, :, :, lanes],
                    slot_sems.at[row, step],
                )
                for columns, lanes in [
                    (columns_of, slice(0, breadth)),
                    (functools.partial(outer_columns, at_core=at_core), side_block),
                ]
            ]
            for step in range(chips)
        ]

    def whole(ref, sem):
        pltpu.make_async_copy(ref, ref, sem).wait()

    give_loads = slot_loads(give, 0, pair - 1 - core)
    mine_loads = slot_loads(mine, 1, core)

    halo_rows = (slice(0, ROWS), slice(ROWS + height, extended))
    barrier = pltpu.get_barrier_semaphore()
    for side in (0, 1):
        @pl.when(has_row[side])
        def _():
            pl.semaphore_signal(barrier, inc=1, device_id=row_device[side], device_id_type=MESH)
    for by in range(1, group):
        pl.semaphore_signal(
            barrier, inc=1, device_id=(w, lax.rem(n + by, group)), device_id_type=MESH
        )
    for load in give_loads[0] + mine_loads[0] + small + sum(give_loads[1:] + mine_loads[1:], []):
        load.start()

    arrivals = group - 1 + has_row[0].astype(jnp.int32) + has_row[1].astype(jnp.int32)
    pl.semaphore_wait(barrier, arrivals)

    def near_copy(step, i):
        return remote(
            give.at[step, :, parts[i], :],
            near.at[step, :, parts[i], :],
            near_sems.at[4 * step],
            near_sems.at[4 * step + 1 + (i if step < chips - 1 else 0)],
            partner,
        )

    def far_copy(step, name):
        kind, rows, side = name
        if kind == "edge":
            lanes = edge[side]
        elif kind == "outer":
            lanes = side_block
        else:
            lanes = slice(LANES, breadth - LANES)
        spot = (slice(None), rows, lanes)
        at = far_groups.index((kind, rows))
        return remote(
            mixed.at[(step, *spot)],
            far.at[(step, *spot)],
            far_sems.at[step, len(far_groups) + int(kind == "outer")],
            far_sems.at[step, at],
            (w, order[step] * pair + core),
        )

    def rims_of(rows):
        return [("edge", rows, 0), ("edge", rows, 1), ("outer", rows, 0)]

    def main_of(rows):
        return ("main", rows, 0)

    far_names = []
    for i in (0, 1):
        far_names += rims_of(rim[i])
    far_names += [main_of(rim[i]) for i in (0, 1)]
    early = len(far_names)
    for i in (0, 1):
        far_names += rims_of(inward[i])
    far_names += [main_of(second[i]) for i in (0, 1)]
    far_names += rims_of(core_rows)
    far_names += [main_of(third[i]) for i in (0, 1)]
    far_names += [main_of(core_rows)]

    far_groups = []
    for kind, rows, _ in far_names:
        if (kind, rows) not in far_groups:
            far_groups.append((kind, rows))

    def far_start(step, name):
        if name[0] == "outer":
            pl.when(has_outer(order[step] * pair + core))(far_copy(step, name).start)
        else:
            far_copy(step, name).start()

    for step in range(chips):
        whole(give.at[step], slot_sems.at[0, step])
        for i in range(3):
            near_copy(step, i).start()

    inner_edge = pl.ds(pl.multiple_of((1 - core) * (breadth - LANES), LANES), LANES)
    outer_edge = pl.ds(pl.multiple_of(core * (breadth - LANES), LANES), LANES)
    def near_edge(side, first, last):
        if side == 0:
            return slice(ROWS + first, ROWS + last), slice(
                ROWS + height + first, ROWS + height + last
            )
        return slice(ROWS + height - last, ROWS + height - first), slice(ROWS - last, ROWS - first)

    def fixed_row(side):
        source, target = near_edge(side, 0, ROWS - 2)
        return remote(
            fixed.at[:, source, 0:breadth],
            fixed.at[:, target, 0:breadth],
            fixed_sems.at[0, side],
            fixed_sems.at[1, 1 - side],
            row_device[side],
        )

    def fixed_column():
        return remote(
            fixed.at[:, own, inner_edge],
            fixed_inner,
            fixed_sems.at[0, 2],
            fixed_sems.at[1, 2],
            partner,
        )

    def given_column():
        return remote(
            given.at[:, own, inner_edge],
            given_inner,
            given_sems.at[0, 2],
            given_sems.at[1, 2],
            partner,
        )

    def outer_column():
        return remote(
            outer_send,
            outer_recv,
            fixed_sems.at[0, 3],
            fixed_sems.at[1, 3],
            (w, n - 1 + 2 * core),
        )

    def fixed_corner(side):
        source, target = near_edge(side, 0, ROWS - 2)
        return remote(
            fixed.at[:, source, side_block],
            fixed.at[:, target, side_block],
            fixed_sems.at[0, side],
            fixed_sems.at[1, 1 - side],
            row_device[side],
        )

    def given_row(side):
        source, target = near_edge(side, 0, 2 * (STEPS - 1))
        return remote(
            given.at[layers, source, :],
            given.at[layers, target, :],
            given_sems.at[0, side],
            given_sems.at[1, 1 - side],
            row_device[side],
        )

    def final_row(side):
        source, target = near_edge(side, 0, 2)
        return remote(
            given.at[0:layers, source, :],
            given.at[0:layers, target, :],
            given_sems.at[0, side],
            given_sems.at[1, 1 - side],
            row_device[side],
        )

    def fixed_both(side):
        source, target = near_edge(side, 0, ROWS - 2)
        return remote(
            fixed.at[:, source, :],
            fixed.at[:, target, :],
            fixed_sems.at[0, side],
            fixed_sems.at[1, 1 - side],
            row_device[side],
        )

    def given_both(side):
        count = 2 * (STEPS - 1) + 2 * layers
        return remote(
            given.at[0, 0:count, :],
            given.at[0, 0:count, :],
            given_sems.at[0, side],
            given_sems.at[1, 1 - side],
            row_device[side],
        )

    def start(has, *makers):
        for side in (0, 1):
            @pl.when(has[side])
            def _():
                for maker in makers:
                    maker(side).start()

    def arrived(has, *makers):
        for side in (0, 1):
            @pl.when(has[side])
            def _():
                for maker in makers:
                    maker(1 - side).wait_recv()

    whole(fixed.at[:, own, 0:breadth], load_sems.at[3])
    for r in range(0, height, ROWS):
        fixed[2, ROWS + r : 2 * ROWS + r, 0:breadth] = sea_ref[r : r + ROWS, :].astype(jnp.float32)

    start(has_row, fixed_row)
    fixed_column().start()
    whole(given.at[:, own, 0:breadth], load_sems.at[4])
    given_column().start()
    shared = [(fixed, i) for i in range(3)] + [(given, i) for i in range(layers + 1)]
    lane = lax.broadcasted_iota(jnp.int32, (ROWS, LANES), 1)
    for r in range(0, height, ROWS):
        packed = jnp.zeros((ROWS, LANES), jnp.float32)
        for a, (ref, i) in enumerate(shared):
            moved = pltpu.roll(ref[i, ROWS + r : 2 * ROWS + r, outer_edge], SHARE * (a + core), 1)
            mine_lanes = jnp.logical_and(lane >= SHARE * a, lane < SHARE * (a + 1))
            packed = jnp.where(mine_lanes, moved, packed)
        outer_send[r : r + ROWS, :] = packed
    pl.when(has_outer(n))(outer_column().start)

    small[0].wait()

    def mix(step, k, rows, lanes):
        mixed[step, k, rows, lanes] = jnp.where(
            owner_ref[k] == n, mine[step, k, rows, lanes], near[step, k, rows, lanes]
        )

    def blocks_of(rows):
        return [slice(r, r + ROWS) for r in range(rows.start, rows.stop, ROWS)]

    everything = slice(0, width)
    for step in range(chips - 1):
        whole(mine.at[step], slot_sems.at[1, step])
        for i in range(3):
            near_copy(step, i).wait_recv()
            for k in range(layers):
                for rows in blocks_of(parts[i]):
                    mix(step, k, rows, everything)
            if i == 1:
                for name in far_names[:early]:
                    far_start(step, name)
            elif i == 2:
                for name in far_names[early:]:
                    far_start(step, name)

    zeros = jnp.zeros((ROWS, width), jnp.float32)
    tile_zeros = jnp.zeros((tiles + 1, ROWS, LANES), jnp.float32)
    for side in (0, 1):
        @pl.when(jnp.logical_not(has_row[side]))
        def _():
            for i in range(3):
                fixed[i, halo_rows[side], :] = zeros
            for i in range(layers + 1):
                given[i, halo_rows[side], :] = zeros
            inner = slice(ROWS + halo_rows[side].start, ROWS + halo_rows[side].stop)
            for k in range(layers):
                field[0, k, :, inner, :] = tile_zeros
                grad[STEPS - 1, k, :, inner, :] = tile_zeros

    for past in (slice(0, ROWS), slice(extended + ROWS, extended + 2 * ROWS)):
        for step in range(STEPS):
            for k in range(layers):
                field[step, k, :, past, :] = tile_zeros
                grad[step, k, :, past, :] = tile_zeros
        for t in range(4):
            wr[t, :, past, :] = tile_zeros

    last = chips - 1
    whole(mine.at[last], slot_sems.at[1, last])
    remote(
        give.at[last], near.at[last], near_sems.at[4 * last], near_sems.at[4 * last + 1], partner
    ).wait_recv()

    small[1].wait()
    small[2].wait()
    speeds = []
    for k in range(layers):
        total = 0.0
        for c in range(speed_ref.shape[0]):
            total = jnp.where(class_ref[k] == c, speed_ref[c], total)
        speeds.append(total)

    upper = (lane >= LANES // 2).astype(jnp.int32)
    fixed_column().wait_recv()
    given_column().wait_recv()
    pl.when(has_outer(n))(outer_column().wait_recv)
    for a, (ref, i) in enumerate(shared):
        inner_ref = (fixed_inner, given_inner)[a >= 3]
        for r in range(0, height, ROWS):
            rows = slice(r, r + ROWS)
            back_by = lax.rem(2 * LANES - SHARE * (a + 1 - core), LANES)
            outer = jnp.where(has_outer(n), pltpu.roll(outer_recv[rows, :], back_by, 1), 0.0)
            ref[i, ROWS + r : 2 * ROWS + r, side_block] = jnp.where(
                upper == core, inner_ref[i, rows, :], outer
            )
    start(has_row, fixed_corner, final_row, given_row)

    def tiled(value):
        return jnp.stack(
            [value[:, j * LANES : (j + 1) * LANES] for j in range(value.shape[1] // LANES)]
        )

    wide_lane = lax.broadcasted_iota(jnp.int32, (tiles + 1, ROWS, LANES), 2)

    def columns_off(value, offset):
        turned = pltpu.roll(value, (-offset) % LANES, 2)
        if offset > 0:
            beside = jnp.concatenate([turned[1:], turned[:1]], axis=0)
            return jnp.where(wide_lane < LANES - offset, turned, beside)
        beside = jnp.concatenate([turned[-1:], turned[:-1]], axis=0)
        return jnp.where(wide_lane >= -offset, turned, beside)

    def make_weights(b):
        rows = slice(b * ROWS, (b + 1) * ROWS)
        inner = slice((b + 1) * ROWS, (b + 2) * ROWS)
        row_w = stencil_weights(tiled(fixed[0, rows, :]))
        col_w = stencil_weights(tiled(fixed[1, rows, :]))
        for t, offset in enumerate(OFFSETS):
            wr[t, :, inner, :] = row_w[offset + 2]
            wc[t, :, rows, :] = col_w[offset + 2]
            wc_back[3 - t, :, rows, :] = columns_off(col_w[offset + 2], -offset)
        centre[:, rows, :] = 1.0 + row_w[2] + col_w[2]
        sea[:, rows, :] = tiled(fixed[2, rows, :])

    def turn_weights(b):
        for t, offset in enumerate(OFFSETS):
            base = (b + 1) * ROWS + offset
            wr_back[t, :, b * ROWS : (b + 1) * ROWS, :] = wr[3 - t, :, base : base + ROWS, :]

    for b in all_blocks[1:-1]:
        make_weights(b)

    def mask_given(b):
        rows = slice(b * ROWS, (b + 1) * ROWS)
        mask = sea[:, rows, :]
        for k in range(layers):
            final_masked[k, :, rows, :] = mask * tiled(given[k, rows, :])
        deposit_masked[:, rows, :] = mask * tiled(given[layers, rows, :])

    for b in inside:
        turn_weights(b)
    for b in all_blocks[1:-1]:
        mask_given(b)

    def chosen(k, rows, lanes):
        value = jnp.where(
            owner_ref[k] == n, mine[last, k, rows, lanes], near[last, k, rows, lanes]
        )
        for step in range(chips - 1):
            sender = lax.rem(chip + chips - 1 - step, chips)
            value = jnp.where(
                lax.div(owner_ref[k], pair) == sender, far[step, k, rows, lanes], value
            )
        return value

    def put(rows, lanes):
        for k in range(layers):
            for piece in halves_of(rows):
                value = chosen(k, piece, lanes)
                for j in range(value.shape[1] // LANES):
                    field[0, k, lanes.start // LANES + j, shifted(piece), :] = value[
                        :, j * LANES : (j + 1) * LANES
                    ]

    def halves_of(rows):
        return [slice(r, r + HALF) for r in range(rows.start, rows.stop, HALF)]

    def shifted(rows):
        return slice(2 * ROWS + rows.start, 2 * ROWS + rows.stop)

    swaps = [*rim, *inward, core_rows]

    def field_column(rows):
        at = swaps.index(rows)
        return remote(
            field.at[0, :, (1 - core) * (tiles - 1), shifted(rows), :],
            field_inner.at[:, rows, :],
            col_sems.at[len(swaps)],
            col_sems.at[at],
            partner,
        )

    halo_near = (
        slice(2 * ROWS - HALF, 2 * ROWS),
        slice(2 * ROWS + height, 2 * ROWS + height + HALF),
    )
    halo_beyond = (
        slice(ROWS, 2 * ROWS - HALF),
        slice(2 * ROWS + height + HALF, 3 * ROWS + height),
    )

    def field_row(side):
        return remote(
            field.at[0, :, 0:tiles, shifted(rim[side]), :],
            field.at[0, :, 0:tiles, halo_near[1 - side], :],
            row_sems.at[0, side],
            row_sems.at[1, 1 - side],
            row_device[side],
        )

    def field_corner(side):
        return remote(
            field.at[0, :, tiles, shifted(rim[side]), :],
            field.at[0, :, tiles, halo_near[1 - side], :],
            row_sems.at[0, side],
            row_sems.at[1, 1 - side],
            row_device[side],
        )

    def field_both(side):
        return remote(
            field.at[0, :, :, shifted(rim[side]), :],
            field.at[0, :, :, halo_near[1 - side], :],
            row_sems.at[0, side],
            row_sems.at[1, 1 - side],
            row_device[side],
        )

    def late_row(side):
        return remote(
            field.at[0, :, :, shifted(second[side]), :],
            field_late.at[1 - side],
            round_sems.at[0, side],
            late_sems.at[1 - side],
            row_device[side],
        )

    def start_row(side, maker):
        pl.when(has_row[side])(maker(side).start)

    def take(name):
        for step in range(chips - 1):
            if name[0] == "outer":
                pl.when(has_outer(n))(far_copy(step, name).wait_recv)
            else:
                far_copy(step, name).wait_recv()

    def take_edges(rows):
        for step in range(chips - 1):
            spot = (step, slice(None), rows, slice(0, 2 * LANES))
            remote(
                mixed.at[spot],
                far.at[spot],
                far_sems.at[step, len(far_groups)],
                far_sems.at[step, far_groups.index(("edge", rows))],
                (w, order[step] * pair + core),
            ).wait_recv()

    def put_outer(rows):
        for k in range(layers):
            for piece in halves_of(rows):
                value = chosen(k, piece, side_block)
                field_outer[k, piece, :] = jnp.where(has_outer(n), value, 0.0)

    def join_field(rows):
        field_column(rows).wait_recv()
        for k in range(layers):
            for piece in halves_of(rows):
                field[0, k, tiles, shifted(piece), :] = jnp.where(
                    upper[:HALF] == core, field_inner[k, piece, :], field_outer[k, piece, :]
                )

    def take_rims(rows):
        take_edges(rows)
        for side in (0, 1):
            put(rows, edge[side])
        field_column(rows).start()
        take(("outer", rows, 0))
        put_outer(rows)

    def take_main(rows):
        take(main_of(rows))
        put(rows, slice(LANES, breadth - LANES))

    for i in (0, 1):
        take_rims(rim[i])
    for i in (0, 1):
        take_main(rim[i])
        start_row(i, field_row)
        join_field(rim[i])
        start_row(i, field_corner)
    for i in (0, 1):
        take_rims(inward[i])
    for i in (0, 1):
        take_main(second[i])
        join_field(inward[i])
        start_row(i, late_row)
    arrived(has_row, fixed_both)
    make_weights(0)
    make_weights(all_blocks[-1])
    take_rims(core_rows)
    chunks = [slice(j, min(j + CHUNK, tiles + 1)) for j in range(0, tiles + 1, CHUNK)]

    class Block:
        def __init__(self, b):
            self.first = b * ROWS

        def load(self, ref, c, above=0, off=0):
            first = self.first + above + off
            return ref[c, first : first + ROWS, :]

        def store(self, ref, c, value, above=0):
            first = self.first + above
            ref[c, first : first + ROWS, :] = value

        def out(self, k, j, value):
            first = self.first - ROWS
            out_ref[k, first : first + ROWS, j * LANES : (j + 1) * LANES] = value

    class Pair:
        def __init__(self, depth):
            self.top = ROWS + depth
            self.bottom = ROWS + height - depth - HALF

        def load(self, ref, c, above=0, off=0):
            top = self.top + above + off
            bottom = self.bottom + above + off - HALF
            upper_rows = ref[c, top : top + ROWS, :]
            sub = lax.broadcasted_iota(jnp.int32, upper_rows.shape, 1)
            return jnp.where(sub < HALF, upper_rows, ref[c, bottom : bottom + ROWS, :])

        def store(self, ref, c, value, above=0):
            top, bottom = self.top + above, self.bottom + above
            ref[c, top : top + HALF, :] = value[:, :HALF, :]
            ref[c, bottom : bottom + HALF, :] = value[:, HALF:, :]

        def out(self, k, j, value):
            top, bottom = self.top - ROWS, self.bottom - ROWS
            lanes = slice(j * LANES, (j + 1) * LANES)
            out_ref[k, top : top + HALF, lanes] = value[:HALF, :]
            out_ref[k, bottom : bottom + HALF, lanes] = value[HALF:, :]

    chunks = [slice(j, min(j + CHUNK, tiles + 1)) for j in range(0, tiles + 1, CHUNK)]
    full = slice(0, tiles + 1)

    def stencils(sources, spot, rows_ref, rows_above, cols_ref):
        here = [spot.load(source, full, ROWS) for source in sources]
        moved = [[columns_off(value, o) for o in OFFSETS] for value in here]
        for c in chunks:
            rows_w = [spot.load(rows_ref.at[t], c, rows_above) for t in range(4)]
            cols_w = [spot.load(cols_ref.at[t], c) for t in range(4)]
            middle = spot.load(centre, c)
            totals = []
            for k, source in enumerate(sources):
                total = middle * here[k][c]
                for t, o in enumerate(OFFSETS):
                    total += rows_w[t] * spot.load(source, c, ROWS, o)
                    total += cols_w[t] * moved[k][t][c]
                totals.append(total)
            yield c, totals

    def forward(step, spot):
        sources = [field.at[step, k] for k in range(layers)]
        for c, totals in stencils(sources, spot, wr, ROWS, wc):
            above = None
            for k, adv in enumerate(totals):
                part = 1.0 / (1.0 + adv * adv)
                settled = speeds[k] * part
                spot.store(slope.at[step, k], c, settled * (2.0 * part - 1.0))
                if step + 1 < STEPS:
                    flux = settled * adv
                    left = adv - flux
                    if above is not None:
                        left = left + above
                    spot.store(field.at[step + 1, k], c, left * spot.load(sea, c), ROWS)
                    above = flux

    def settle_back(step, spot, c, masked, keep):
        below = spot.load(deposit_masked, c)
        for k in reversed(range(layers)):
            keep(k, c, masked[k] + (below - masked[k]) * spot.load(slope.at[step, k], c))
            below = masked[k]

    def keep_grad(step, spot):
        def keep(k, c, value):
            spot.store(grad.at[step, k], c, value, ROWS)

        return keep

    def back(step, spot):
        sources = [grad.at[step, k] for k in range(layers)]
        for c, adjoint in stencils(sources, spot, wr_back, 0, wc_back):
            if step:
                mask = spot.load(sea, c)
                masked = [value * mask for value in adjoint]
                settle_back(step - 1, spot, c, masked, keep_grad(step - 1, spot))
            else:
                for k in range(layers):
                    for j in range(c.start, min(c.stop, tiles)):
                        spot.out(k, j, adjoint[k][j - c.start])

    final_step = STEPS - 1

    def last_forward(spot, keep):
        forward(final_step, spot)
        for c in chunks:
            masked = [spot.load(final_masked.at[k], c) for k in range(layers)]
            settle_back(final_step, spot, c, masked, keep)

    def round_copy(side):
        return remote(
            round_send.at[side],
            round_recv.at[1 - side],
            round_sems.at[0, side],
            round_sems.at[1, 1 - side],
            row_device[side],
        )

    def round_both(side):
        return remote(
            round_send,
            round_recv,
            round_sems.at[0, side],
            round_sems.at[1, 1 - side],
            row_device[side],
        )

    def receive_round(side):
        first = 2 * ROWS - 2 - HALF if side == 0 else 2 * ROWS + height + 2

        @pl.when(has_row[side])
        def _():
            round_copy(1 - side).wait_recv()
            for k in range(layers):
                grad[final_step, k, :, first : first + HALF, :] = round_recv[side, k]

    arrived(has_row, field_both)
    for b in (all_blocks[0], all_blocks[-1]):
        forward(0, Block(b))
    for side in (0, 1):
        b = all_blocks[-2] if side else all_blocks[1]
        take_main(third[side])
        forward(0, Block(b))
        forward(0, Block(b + 1 - 2 * side))
        for step in range(1, final_step):
            forward(step, Block(b))
        first = 2 if side == 0 else ROWS - 2 - HALF

        def keep_round(k, c, value):
            round_send[side, k, c] = value[:, first : first + HALF, :]

        last_forward(Block(b), keep_round)
        start_row(side, round_copy)

    take_main(core_rows)
    join_field(core_rows)
    for step in range(final_step):
        for b in inside:
            forward(step, Block(b))
    for b in inside:
        last_forward(Block(b), keep_grad(final_step, Block(b)))
    def left(has, *makers):
        for side in (0, 1):
            @pl.when(has[side])
            def _():
                for maker in makers:
                    maker(side).wait_send()

    for step in range(chips):
        remote(
            give.at[step], near.at[step], near_sems.at[4 * step], near_sems.at[4 * step + 1], partner
        ).wait_send()
    for step in range(chips - 1):
        device = order[step] * pair + core
        for i, lanes in enumerate((slice(0, breadth), side_block)):
            sent = remote(
                mixed.at[step, :, :, lanes],
                far.at[step, :, :, lanes],
                far_sems.at[step, len(far_groups) + i],
                far_sems.at[step, 0],
                (w, device),
            )
            if i == 0:
                sent.wait_send()
            else:
                pl.when(has_outer(device))(sent.wait_send)
    remote(
        field.at[0, :, (1 - core) * (tiles - 1), shifted(slice(0, height)), :],
        field_inner,
        col_sems.at[len(swaps)],
        col_sems.at[0],
        partner,
    ).wait_send()
    fixed_column().wait_send()
    given_column().wait_send()
    pl.when(has_outer(n))(outer_column().wait_send)
    left(has_row, fixed_both, given_both, field_both)

    for side in (0, 1):
        @pl.when(has_row[side])
        def _():
            late_row(1 - side).wait_recv()
            for k in range(layers):
                field[0, k, :, halo_beyond[side], :] = field_late[side, k]

    ends = (all_blocks[0], all_blocks[-1])
    for step in range(final_step):
        for b in ends:
            forward(step, Block(b))
    arrived(has_row, given_both)
    for b in ends:
        mask_given(b)
    for b in (all_blocks[1], all_blocks[-2]):
        last_forward(Block(b), keep_grad(final_step, Block(b)))
    last_forward(Pair(-HALF), keep_grad(final_step, Pair(-HALF)))
    for b in (*all_blocks[:2], *all_blocks[-2:]):
        turn_weights(b)

    for step in range(final_step, -1, -1):
        for b in all_blocks[1:-1]:
            back(step, Block(b))
    for side in (0, 1):
        receive_round(side)
    for step in range(final_step, -1, -1):
        back(step, Pair(-2 * step))

    left(has_row, round_both)


def body(group_wide, group, slots, owner, row_v, col_v, land_sea, layer_class, speed, final, deposit):
    layers, height, breadth = final.shape
    chips = group // 2
    hops = max(chips - 1, 1)
    f32 = jnp.float32
    extended = height + 2 * ROWS
    padded = extended + 2 * ROWS
    width = breadth + LANES
    tiles = width // LANES
    dma = pltpu.SemaphoreType.DMA
    vmem = pl.BlockSpec(memory_space=pltpu.VMEM)
    hbm = pl.BlockSpec(memory_space=pltpu.HBM)
    return pl.pallas_call(
        functools.partial(kernel, group_wide, group),
        out_shape=pltpu.VMEM(final.shape, f32),
        in_specs=[hbm] * 9,
        out_specs=vmem,
        scratch_shapes=[
            pltpu.SMEM(owner.shape, owner.dtype),
            pltpu.SMEM(layer_class.shape, layer_class.dtype),
            pltpu.SMEM(speed.shape, speed.dtype),
            pltpu.VMEM(land_sea.shape, land_sea.dtype),
            pltpu.VMEM((3, extended, width), f32),
            pltpu.VMEM((3, height, LANES), f32),
            pltpu.VMEM((layers + 1, extended, width), f32),
            pltpu.VMEM((layers + 1, height, LANES), f32),
            pltpu.VMEM((height, LANES), f32),
            pltpu.VMEM((height, LANES), f32),
            pltpu.VMEM((chips, layers, height, width), f32),
            pltpu.VMEM((chips, layers, height, width), f32),
            pltpu.VMEM((chips, layers, height, width), f32),
            pltpu.VMEM((hops, layers, height, width), f32),
            pltpu.VMEM((hops, layers, height, width), f32),
            pltpu.VMEM((STEPS, layers, tiles, padded, LANES), f32),
            pltpu.VMEM((layers, height, LANES), f32),
            pltpu.VMEM((layers, height, LANES), f32),
            pltpu.VMEM((2, layers, tiles, HALF, LANES), f32),
            pltpu.VMEM((STEPS, layers, tiles, extended, LANES), f32),
            pltpu.VMEM((STEPS, layers, tiles, padded, LANES), f32),
            pltpu.VMEM((4, tiles, padded, LANES), f32),
            pltpu.VMEM((4, tiles, extended, LANES), f32),
            pltpu.VMEM((4, tiles, extended, LANES), f32),
            pltpu.VMEM((4, tiles, extended, LANES), f32),
            pltpu.VMEM((tiles, extended, LANES), f32),
            pltpu.VMEM((tiles, extended, LANES), f32),
            pltpu.VMEM((layers, tiles, extended, LANES), f32),
            pltpu.VMEM((tiles, extended, LANES), f32),
            pltpu.VMEM((2, layers, tiles, HALF, LANES), f32),
            pltpu.VMEM((2, layers, tiles, HALF, LANES), f32),
            dma((5,)),
            dma((2, chips)),
            dma((4 * (chips - 1) + 2,)),
            dma((hops, 17 + 2)),
            dma((2, 4)),
            dma((2, 3)),
            dma((6,)),
            dma((2, 2)),
            dma((2,)),
            dma((2, 2)),
        ],
        compiler_params=pltpu.CompilerParams(
            collective_id=0,
            has_side_effects=True,
            vmem_limit_bytes=VMEM_BYTES - final.size * final.dtype.itemsize,
        ),
    )(owner, layer_class, speed, slots, row_v, col_v, land_sea, final, deposit)


def solution(mesh):
    in_specs = (
        P("narrow", None, "wide", None),
        P(),
        P("wide", "narrow"),
        P("wide", "narrow"),
        P("wide", "narrow"),
        P(),
        P(),
        P(None, "wide", "narrow"),
        P("wide", "narrow"),
    )
    out_specs = P(None, "wide", "narrow")
    return jax.shard_map(
        functools.partial(body, mesh.shape["wide"], mesh.shape["narrow"]),
        mesh=mesh,
        in_specs=in_specs,
        out_specs=out_specs,
        check_vma=False,
    )
```

```python
import functools

import jax
import jax.numpy as jnp
from jax import lax
from jax.experimental import pallas as pl
from jax.experimental.pallas import tpu as pltpu
from jax.sharding import PartitionSpec as P

STEPS = 3
LANES = 128
ROWS = 8
HALF = ROWS // 2
SHARE = 16
CHUNK = 3
OFFSETS = (-2, -1, 1, 2)
MESH = pl.DeviceIdType.MESH
VMEM_BYTES = 67043328


def stencil_weights(velocity):
    p = jnp.maximum(velocity, 0.0)
    q = jnp.minimum(velocity, 0.0)
    pp = p * p
    qq = q * q
    return [
        0.5 * pp - 0.5 * p,
        2.0 * p - pp,
        0.5 * pp - 1.5 * p + 0.5 * qq + 1.5 * q,
        -2.0 * q - qq,
        0.5 * qq + 0.5 * q,
    ]


def kernel(
    group_wide,
    group,
    owner_hbm,
    class_hbm,
    speed_hbm,
    slots_hbm,
    row_velocity_hbm,
    column_velocity_hbm,
    sea_hbm,
    final_hbm,
    deposit_hbm,
    out_ref,
    owner_ref,
    class_ref,
    speed_ref,
    sea_ref,
    fixed,
    fixed_inner,
    given,
    given_inner,
    outer_send,
    outer_recv,
    mine,
    give,
    near,
    mixed,
    far,
    field,
    field_inner,
    field_outer,
    field_late,
    slope,
    grad,
    wr,
    wc,
    wr_back,
    wc_back,
    centre,
    sea,
    final_masked,
    deposit_masked,
    round_send,
    round_recv,
    load_sems,
    slot_sems,
    near_sems,
    far_sems,
    fixed_sems,
    given_sems,
    col_sems,
    row_sems,
    late_sems,
    round_sems,
):
    layers, height, breadth = out_ref.shape
    pair = 2
    chips = group // pair
    w = lax.axis_index("wide")
    n = lax.axis_index("narrow")
    chip = lax.div(n, pair)
    core = lax.rem(n, pair)
    width = breadth + LANES
    tiles = breadth // LANES
    own_blocks = height // ROWS
    extended = height + 2 * ROWS
    all_blocks = list(range(own_blocks + 2))
    inside = all_blocks[2:-2]
    edge = (slice(0, LANES), slice(breadth - LANES, breadth))
    side_block = slice(breadth, width)
    own = slice(ROWS, ROWS + height)

    has_row = (w > 0, w < group_wide - 1)
    row_device = ((w - 1, n), (w + 1, n))
    partner = (w, chip * pair + (pair - 1 - core))
    order = [lax.rem(chip + by, chips) for by in range(1, chips)] + [chip]
    parts = (
        slice(0, ROWS),
        slice(height - ROWS, height),
        slice(ROWS, height - ROWS),
    )
    def pieces_at(first, last):
        return (slice(first, last), slice(height - last, height - first))

    rim = pieces_at(0, HALF)
    second = pieces_at(HALF, 2 * HALF)
    third = pieces_at(2 * HALF, 3 * HALF)
    inward = pieces_at(HALF, 3 * HALF)
    core_rows = slice(3 * HALF, height - 3 * HALF)

    def columns_of(device):
        return pl.ds(pl.multiple_of(device * breadth, LANES), breadth)

    def outer_columns(device, at_core):
        start = device * breadth - LANES + at_core * (breadth + LANES)
        return pl.ds(pl.multiple_of(lax.rem(start + group * breadth, group * breadth), LANES), LANES)

    def has_outer(device):
        beside = device - 1 + 2 * core
        return jnp.logical_and(beside >= 0, beside < group)

    def remote(src, dst, send_sem, recv_sem, device):
        return pltpu.make_async_remote_copy(
            src_ref=src,
            dst_ref=dst,
            send_sem=send_sem,
            recv_sem=recv_sem,
            device_id=device,
            device_id_type=MESH,
        )

    small = [
        pltpu.make_async_copy(source, target, load_sems.at[(0, 1, 2, 3, 3, 3, 4, 4)[i]])
        for i, (source, target) in enumerate(
            [
                (owner_hbm, owner_ref),
                (class_hbm, class_ref),
                (speed_hbm, speed_ref),
                (sea_hbm, sea_ref),
                (row_velocity_hbm, fixed.at[0, own, 0:breadth]),
                (column_velocity_hbm, fixed.at[1, own, 0:breadth]),
                (final_hbm, given.at[0:layers, own, 0:breadth]),
                (deposit_hbm, given.at[layers, own, 0:breadth]),
            ]
        )
    ]
    def slot_loads(target, row, at_core):
        return [
            [
                pltpu.make_async_copy(
                    slots_hbm.at[0, :, :, columns(order[step] * pair + at_core)],
                    target.at[step, :, :, lanes],
                    slot_sems.at[row, step],
                )
                for columns, lanes in [
                    (columns_of, slice(0, breadth)),
                    (functools.partial(outer_columns, at_core=at_core), side_block),
                ]
            ]
            for step in range(chips)
        ]

    def whole(ref, sem):
        pltpu.make_async_copy(ref, ref, sem).wait()

    give_loads = slot_loads(give, 0, pair - 1 - core)
    mine_loads = slot_loads(mine, 1, core)

    halo_rows = (slice(0, ROWS), slice(ROWS + height, extended))
    barrier = pltpu.get_barrier_semaphore()
    for side in (0, 1):
        @pl.when(has_row[side])
        def _():
            pl.semaphore_signal(barrier, inc=1, device_id=row_device[side], device_id_type=MESH)
    for by in range(1, group):
        pl.semaphore_signal(
            barrier, inc=1, device_id=(w, lax.rem(n + by, group)), device_id_type=MESH
        )
    for load in give_loads[0] + mine_loads[0] + small + sum(give_loads[1:] + mine_loads[1:], []):
        load.start()

    arrivals = group - 1 + has_row[0].astype(jnp.int32) + has_row[1].astype(jnp.int32)
    pl.semaphore_wait(barrier, arrivals)

    def near_copy(step, i):
        return remote(
            give.at[step, :, parts[i], :],
            near.at[step, :, parts[i], :],
            near_sems.at[4 * step],
            near_sems.at[4 * step + 1 + (i if step < chips - 1 else 0)],
            partner,
        )

    def far_copy(step, name):
        kind, rows, side = name
        if kind == "edge":
            lanes = edge[side]
        elif kind == "outer":
            lanes = side_block
        else:
            lanes = slice(LANES, breadth - LANES)
        spot = (slice(None), rows, lanes)
        at = far_groups.index((kind, rows))
        return remote(
            mixed.at[(step, *spot)],
            far.at[(step, *spot)],
            far_sems.at[step, len(far_groups) + int(kind == "outer")],
            far_sems.at[step, at],
            (w, order[step] * pair + core),
        )

    def rims_of(rows):
        return [("edge", rows, 0), ("edge", rows, 1), ("outer", rows, 0)]

    def main_of(rows):
        return ("main", rows, 0)

    far_names = []
    for i in (0, 1):
        far_names += rims_of(rim[i])
    far_names += [main_of(rim[i]) for i in (0, 1)]
    early = len(far_names)
    for i in (0, 1):
        far_names += rims_of(inward[i])
    far_names += [main_of(second[i]) for i in (0, 1)]
    far_names += rims_of(core_rows)
    far_names += [main_of(third[i]) for i in (0, 1)]
    far_names += [main_of(core_rows)]

    far_groups = []
    for kind, rows, _ in far_names:
        if (kind, rows) not in far_groups:
            far_groups.append((kind, rows))

    def far_start(step, name):
        if name[0] == "outer":
            pl.when(has_outer(order[step] * pair + core))(far_copy(step, name).start)
        else:
            far_copy(step, name).start()

    for step in range(chips):
        whole(give.at[step], slot_sems.at[0, step])
        for i in range(3):
            near_copy(step, i).start()

    inner_edge = pl.ds(pl.multiple_of((1 - core) * (breadth - LANES), LANES), LANES)
    outer_edge = pl.ds(pl.multiple_of(core * (breadth - LANES), LANES), LANES)
    def near_edge(side, first, last):
        if side == 0:
            return slice(ROWS + first, ROWS + last), slice(
                ROWS + height + first, ROWS + height + last
            )
        return slice(ROWS + height - last, ROWS + height - first), slice(ROWS - last, ROWS - first)

    def fixed_row(side):
        source, target = near_edge(side, 0, ROWS - 2)
        return remote(
            fixed.at[:, source, 0:breadth],
            fixed.at[:, target, 0:breadth],
            fixed_sems.at[0, side],
            fixed_sems.at[1, 1 - side],
            row_device[side],
        )

    def fixed_column():
        return remote(
            fixed.at[:, own, inner_edge],
            fixed_inner,
            fixed_sems.at[0, 2],
            fixed_sems.at[1, 2],
            partner,
        )

    def given_column():
        return remote(
            given.at[:, own, inner_edge],
            given_inner,
            given_sems.at[0, 2],
            given_sems.at[1, 2],
            partner,
        )

    def outer_column():
        return remote(
            outer_send,
            outer_recv,
            fixed_sems.at[0, 3],
            fixed_sems.at[1, 3],
            (w, n - 1 + 2 * core),
        )

    def fixed_corner(side):
        source, target = near_edge(side, 0, ROWS - 2)
        return remote(
            fixed.at[:, source, side_block],
            fixed.at[:, target, side_block],
            fixed_sems.at[0, side],
            fixed_sems.at[1, 1 - side],
            row_device[side],
        )

    def given_rows(lanes):
        def deposit_rows(side):
            source, target = near_edge(side, 0, 2 * (STEPS - 1))
            return remote(
                given.at[layers, source, lanes],
                given.at[layers, target, lanes],
                given_sems.at[0, side],
                given_sems.at[1, 1 - side],
                row_device[side],
            )

        def final_rows(side):
            source, target = near_edge(side, 0, 2)
            return remote(
                given.at[0:layers, source, lanes],
                given.at[0:layers, target, lanes],
                given_sems.at[0, side],
                given_sems.at[1, 1 - side],
                row_device[side],
            )

        return final_rows, deposit_rows

    def fixed_both(side):
        source, target = near_edge(side, 0, ROWS - 2)
        return remote(
            fixed.at[:, source, :],
            fixed.at[:, target, :],
            fixed_sems.at[0, side],
            fixed_sems.at[1, 1 - side],
            row_device[side],
        )

    def given_both(side):
        count = 2 * (STEPS - 1) + 2 * layers
        return remote(
            given.at[0, 0:count, :],
            given.at[0, 0:count, :],
            given_sems.at[0, side],
            given_sems.at[1, 1 - side],
            row_device[side],
        )

    def start(has, *makers):
        for side in (0, 1):
            @pl.when(has[side])
            def _():
                for maker in makers:
                    maker(side).start()

    def arrived(has, *makers):
        for side in (0, 1):
            @pl.when(has[side])
            def _():
                for maker in makers:
                    maker(1 - side).wait_recv()

    whole(fixed.at[:, own, 0:breadth], load_sems.at[3])
    for r in range(0, height, ROWS):
        fixed[2, ROWS + r : 2 * ROWS + r, 0:breadth] = sea_ref[r : r + ROWS, :].astype(jnp.float32)

    start(has_row, fixed_row)
    fixed_column().start()
    whole(given.at[:, own, 0:breadth], load_sems.at[4])
    start(has_row, *given_rows(slice(0, breadth)))
    given_column().start()
    shared = [(fixed, i) for i in range(3)] + [(given, i) for i in range(layers + 1)]
    lane = lax.broadcasted_iota(jnp.int32, (ROWS, LANES), 1)
    for r in range(0, height, ROWS):
        packed = jnp.zeros((ROWS, LANES), jnp.float32)
        for a, (ref, i) in enumerate(shared):
            moved = pltpu.roll(ref[i, ROWS + r : 2 * ROWS + r, outer_edge], SHARE * (a + core), 1)
            mine_lanes = jnp.logical_and(lane >= SHARE * a, lane < SHARE * (a + 1))
            packed = jnp.where(mine_lanes, moved, packed)
        outer_send[r : r + ROWS, :] = packed
    pl.when(has_outer(n))(outer_column().start)

    small[0].wait()

    def mix(step, k, rows, lanes):
        mixed[step, k, rows, lanes] = jnp.where(
            owner_ref[k] == n, mine[step, k, rows, lanes], near[step, k, rows, lanes]
        )

    def blocks_of(rows):
        return [slice(r, r + ROWS) for r in range(rows.start, rows.stop, ROWS)]

    everything = slice(0, width)
    for step in range(chips - 1):
        whole(mine.at[step], slot_sems.at[1, step])
        for i in range(3):
            near_copy(step, i).wait_recv()
            for k in range(layers):
                for rows in blocks_of(parts[i]):
                    mix(step, k, rows, everything)
            if i == 1:
                for name in far_names[:early]:
                    far_start(step, name)
            elif i == 2:
                for name in far_names[early:]:
                    far_start(step, name)

    zeros = jnp.zeros((ROWS, width), jnp.float32)
    tile_zeros = jnp.zeros((tiles + 1, ROWS, LANES), jnp.float32)
    for side in (0, 1):
        @pl.when(jnp.logical_not(has_row[side]))
        def _():
            for i in range(3):
                fixed[i, halo_rows[side], :] = zeros
            for i in range(layers + 1):
                given[i, halo_rows[side], :] = zeros
            inner = slice(ROWS + halo_rows[side].start, ROWS + halo_rows[side].stop)
            for k in range(layers):
                field[0, k, :, inner, :] = tile_zeros
                grad[STEPS - 1, k, :, inner, :] = tile_zeros

    for past in (slice(0, ROWS), slice(extended + ROWS, extended + 2 * ROWS)):
        for step in range(STEPS):
            for k in range(layers):
                field[step, k, :, past, :] = tile_zeros
                grad[step, k, :, past, :] = tile_zeros
        for t in range(4):
            wr[t, :, past, :] = tile_zeros

    last = chips - 1
    whole(mine.at[last], slot_sems.at[1, last])
    remote(
        give.at[last], near.at[last], near_sems.at[4 * last], near_sems.at[4 * last + 1], partner
    ).wait_recv()

    small[1].wait()
    small[2].wait()
    speeds = []
    for k in range(layers):
        total = 0.0
        for c in range(speed_ref.shape[0]):
            total = jnp.where(class_ref[k] == c, speed_ref[c], total)
        speeds.append(total)

    upper = (lane >= LANES // 2).astype(jnp.int32)
    fixed_column().wait_recv()
    given_column().wait_recv()
    pl.when(has_outer(n))(outer_column().wait_recv)
    for a, (ref, i) in enumerate(shared):
        inner_ref = (fixed_inner, given_inner)[a >= 3]
        for r in range(0, height, ROWS):
            rows = slice(r, r + ROWS)
            back_by = lax.rem(2 * LANES - SHARE * (a + 1 - core), LANES)
            outer = jnp.where(has_outer(n), pltpu.roll(outer_recv[rows, :], back_by, 1), 0.0)
            ref[i, ROWS + r : 2 * ROWS + r, side_block] = jnp.where(
                upper == core, inner_ref[i, rows, :], outer
            )
    start(has_row, fixed_corner, *given_rows(side_block))

    def tiled(value):
        return jnp.stack(
            [value[:, j * LANES : (j + 1) * LANES] for j in range(value.shape[1] // LANES)]
        )

    wide_lane = lax.broadcasted_iota(jnp.int32, (tiles + 1, ROWS, LANES), 2)

    def columns_off(value, offset):
        turned = pltpu.roll(value, (-offset) % LANES, 2)
        if offset > 0:
            beside = jnp.concatenate([turned[1:], turned[:1]], axis=0)
            return jnp.where(wide_lane < LANES - offset, turned, beside)
        beside = jnp.concatenate([turned[-1:], turned[:-1]], axis=0)
        return jnp.where(wide_lane >= -offset, turned, beside)

    def make_weights(b):
        rows = slice(b * ROWS, (b + 1) * ROWS)
        inner = slice((b + 1) * ROWS, (b + 2) * ROWS)
        row_w = stencil_weights(tiled(fixed[0, rows, :]))
        col_w = stencil_weights(tiled(fixed[1, rows, :]))
        for t, offset in enumerate(OFFSETS):
            wr[t, :, inner, :] = row_w[offset + 2]
            wc[t, :, rows, :] = col_w[offset + 2]
            wc_back[3 - t, :, rows, :] = columns_off(col_w[offset + 2], -offset)
        centre[:, rows, :] = 1.0 + row_w[2] + col_w[2]
        sea[:, rows, :] = tiled(fixed[2, rows, :])

    def turn_weights(b):
        for t, offset in enumerate(OFFSETS):
            base = (b + 1) * ROWS + offset
            wr_back[t, :, b * ROWS : (b + 1) * ROWS, :] = wr[3 - t, :, base : base + ROWS, :]

    for b in all_blocks[1:-1]:
        make_weights(b)

    def mask_given(b):
        rows = slice(b * ROWS, (b + 1) * ROWS)
        mask = sea[:, rows, :]
        for k in range(layers):
            final_masked[k, :, rows, :] = mask * tiled(given[k, rows, :])
        deposit_masked[:, rows, :] = mask * tiled(given[layers, rows, :])

    for b in inside:
        turn_weights(b)
    for b in all_blocks[1:-1]:
        mask_given(b)

    def chosen(k, rows, lanes):
        value = jnp.where(
            owner_ref[k] == n, mine[last, k, rows, lanes], near[last, k, rows, lanes]
        )
        for step in range(chips - 1):
            sender = lax.rem(chip + chips - 1 - step, chips)
            value = jnp.where(
                lax.div(owner_ref[k], pair) == sender, far[step, k, rows, lanes], value
            )
        return value

    def put(rows, lanes):
        for k in range(layers):
            for piece in halves_of(rows):
                value = chosen(k, piece, lanes)
                for j in range(value.shape[1] // LANES):
                    field[0, k, lanes.start // LANES + j, shifted(piece), :] = value[
                        :, j * LANES : (j + 1) * LANES
                    ]

    def halves_of(rows):
        return [slice(r, r + HALF) for r in range(rows.start, rows.stop, HALF)]

    def shifted(rows):
        return slice(2 * ROWS + rows.start, 2 * ROWS + rows.stop)

    swaps = [*rim, *inward, core_rows]

    def field_column(rows):
        at = swaps.index(rows)
        return remote(
            field.at[0, :, (1 - core) * (tiles - 1), shifted(rows), :],
            field_inner.at[:, rows, :],
            col_sems.at[len(swaps)],
            col_sems.at[at],
            partner,
        )

    halo_near = (
        slice(2 * ROWS - HALF, 2 * ROWS),
        slice(2 * ROWS + height, 2 * ROWS + height + HALF),
    )
    halo_beyond = (
        slice(ROWS, 2 * ROWS - HALF),
        slice(2 * ROWS + height + HALF, 3 * ROWS + height),
    )

    def field_row(side):
        return remote(
            field.at[0, :, 0:tiles, shifted(rim[side]), :],
            field.at[0, :, 0:tiles, halo_near[1 - side], :],
            row_sems.at[0, side],
            row_sems.at[1, 1 - side],
            row_device[side],
        )

    def field_corner(side):
        return remote(
            field.at[0, :, tiles, shifted(rim[side]), :],
            field.at[0, :, tiles, halo_near[1 - side], :],
            row_sems.at[0, side],
            row_sems.at[1, 1 - side],
            row_device[side],
        )

    def field_both(side):
        return remote(
            field.at[0, :, :, shifted(rim[side]), :],
            field.at[0, :, :, halo_near[1 - side], :],
            row_sems.at[0, side],
            row_sems.at[1, 1 - side],
            row_device[side],
        )

    def late_row(side):
        return remote(
            field.at[0, :, :, shifted(second[side]), :],
            field_late.at[1 - side],
            round_sems.at[0, side],
            late_sems.at[1 - side],
            row_device[side],
        )

    def start_row(side, maker):
        pl.when(has_row[side])(maker(side).start)

    def take(name):
        for step in range(chips - 1):
            if name[0] == "outer":
                pl.when(has_outer(n))(far_copy(step, name).wait_recv)
            else:
                far_copy(step, name).wait_recv()

    def take_edges(rows):
        for step in range(chips - 1):
            spot = (step, slice(None), rows, slice(0, 2 * LANES))
            remote(
                mixed.at[spot],
                far.at[spot],
                far_sems.at[step, len(far_groups)],
                far_sems.at[step, far_groups.index(("edge", rows))],
                (w, order[step] * pair + core),
            ).wait_recv()

    def put_outer(rows):
        for k in range(layers):
            for piece in halves_of(rows):
                value = chosen(k, piece, side_block)
                field_outer[k, piece, :] = jnp.where(has_outer(n), value, 0.0)

    def join_field(rows):
        field_column(rows).wait_recv()
        for k in range(layers):
            for piece in halves_of(rows):
                field[0, k, tiles, shifted(piece), :] = jnp.where(
                    upper[:HALF] == core, field_inner[k, piece, :], field_outer[k, piece, :]
                )

    def take_rims(rows):
        take_edges(rows)
        for side in (0, 1):
            put(rows, edge[side])
        field_column(rows).start()
        take(("outer", rows, 0))
        put_outer(rows)

    def take_main(rows):
        take(main_of(rows))
        put(rows, slice(LANES, breadth - LANES))

    for i in (0, 1):
        take_rims(rim[i])
    for i in (0, 1):
        take_main(rim[i])
        start_row(i, field_row)
        join_field(rim[i])
        start_row(i, field_corner)
    for i in (0, 1):
        take_rims(inward[i])
    for i in (0, 1):
        take_main(second[i])
        join_field(inward[i])
        start_row(i, late_row)
    arrived(has_row, fixed_both)
    make_weights(0)
    make_weights(all_blocks[-1])
    take_rims(core_rows)
    chunks = [slice(j, min(j + CHUNK, tiles + 1)) for j in range(0, tiles + 1, CHUNK)]

    class Block:
        def __init__(self, b):
            self.first = b * ROWS

        def load(self, ref, c, above=0, off=0):
            first = self.first + above + off
            return ref[c, first : first + ROWS, :]

        def store(self, ref, c, value, above=0):
            first = self.first + above
            ref[c, first : first + ROWS, :] = value

        def out(self, k, j, value):
            first = self.first - ROWS
            out_ref[k, first : first + ROWS, j * LANES : (j + 1) * LANES] = value

    class Pair:
        def __init__(self, depth):
            self.top = ROWS + depth
            self.bottom = ROWS + height - depth - HALF

        def load(self, ref, c, above=0, off=0):
            top = self.top + above + off
            bottom = self.bottom + above + off - HALF
            upper_rows = ref[c, top : top + ROWS, :]
            sub = lax.broadcasted_iota(jnp.int32, upper_rows.shape, 1)
            return jnp.where(sub < HALF, upper_rows, ref[c, bottom : bottom + ROWS, :])

        def store(self, ref, c, value, above=0):
            top, bottom = self.top + above, self.bottom + above
            ref[c, top : top + HALF, :] = value[:, :HALF, :]
            ref[c, bottom : bottom + HALF, :] = value[:, HALF:, :]

        def out(self, k, j, value):
            top, bottom = self.top - ROWS, self.bottom - ROWS
            lanes = slice(j * LANES, (j + 1) * LANES)
            out_ref[k, top : top + HALF, lanes] = value[:HALF, :]
            out_ref[k, bottom : bottom + HALF, lanes] = value[HALF:, :]

    chunks = [slice(j, min(j + CHUNK, tiles + 1)) for j in range(0, tiles + 1, CHUNK)]
    full = slice(0, tiles + 1)

    def stencils(sources, spot, rows_ref, rows_above, cols_ref):
        here = [spot.load(source, full, ROWS) for source in sources]
        moved = [[columns_off(value, o) for o in OFFSETS] for value in here]
        for c in chunks:
            rows_w = [spot.load(rows_ref.at[t], c, rows_above) for t in range(4)]
            cols_w = [spot.load(cols_ref.at[t], c) for t in range(4)]
            middle = spot.load(centre, c)
            totals = []
            for k, source in enumerate(sources):
                total = middle * here[k][c]
                for t, o in enumerate(OFFSETS):
                    total += rows_w[t] * spot.load(source, c, ROWS, o)
                    total += cols_w[t] * moved[k][t][c]
                totals.append(total)
            yield c, totals

    def forward(step, spot):
        sources = [field.at[step, k] for k in range(layers)]
        for c, totals in stencils(sources, spot, wr, ROWS, wc):
            above = None
            for k, adv in enumerate(totals):
                part = 1.0 / (1.0 + adv * adv)
                settled = speeds[k] * part
                spot.store(slope.at[step, k], c, settled * (2.0 * part - 1.0))
                if step + 1 < STEPS:
                    flux = settled * adv
                    left = adv - flux
                    if above is not None:
                        left = left + above
                    spot.store(field.at[step + 1, k], c, left * spot.load(sea, c), ROWS)
                    above = flux

    def settle_back(step, spot, c, masked, keep):
        below = spot.load(deposit_masked, c)
        for k in reversed(range(layers)):
            keep(k, c, masked[k] + (below - masked[k]) * spot.load(slope.at[step, k], c))
            below = masked[k]

    def keep_grad(step, spot):
        def keep(k, c, value):
            spot.store(grad.at[step, k], c, value, ROWS)

        return keep

    def back(step, spot):
        sources = [grad.at[step, k] for k in range(layers)]
        for c, adjoint in stencils(sources, spot, wr_back, 0, wc_back):
            if step:
                mask = spot.load(sea, c)
                masked = [value * mask for value in adjoint]
                settle_back(step - 1, spot, c, masked, keep_grad(step - 1, spot))
            else:
                for k in range(layers):
                    for j in range(c.start, min(c.stop, tiles)):
                        spot.out(k, j, adjoint[k][j - c.start])

    final_step = STEPS - 1

    def last_forward(spot, keep):
        forward(final_step, spot)
        for c in chunks:
            masked = [spot.load(final_masked.at[k], c) for k in range(layers)]
            settle_back(final_step, spot, c, masked, keep)

    def round_copy(side):
        return remote(
            round_send.at[side],
            round_recv.at[1 - side],
            round_sems.at[0, side],
            round_sems.at[1, 1 - side],
            row_device[side],
        )

    def round_both(side):
        return remote(
            round_send,
            round_recv,
            round_sems.at[0, side],
            round_sems.at[1, 1 - side],
            row_device[side],
        )

    def receive_round(side):
        first = 2 * ROWS - 2 - HALF if side == 0 else 2 * ROWS + height + 2

        @pl.when(has_row[side])
        def _():
            round_copy(1 - side).wait_recv()
            for k in range(layers):
                grad[final_step, k, :, first : first + HALF, :] = round_recv[side, k]

    arrived(has_row, field_both)
    forward(0, Pair(-HALF))
    for side in (0, 1):
        b = all_blocks[-2] if side else all_blocks[1]
        take_main(third[side])
        forward(0, Block(b))
        forward(0, Block(b + 1 - 2 * side))
        for step in range(1, final_step):
            forward(step, Block(b))
        first = 2 if side == 0 else ROWS - 2 - HALF

        def keep_round(k, c, value):
            round_send[side, k, c] = value[:, first : first + HALF, :]

        last_forward(Block(b), keep_round)
        start_row(side, round_copy)

    take_main(core_rows)
    join_field(core_rows)
    for step in range(final_step):
        for b in inside:
            forward(step, Block(b))
    for b in inside:
        last_forward(Block(b), keep_grad(final_step, Block(b)))
    def left(has, *makers):
        for side in (0, 1):
            @pl.when(has[side])
            def _():
                for maker in makers:
                    maker(side).wait_send()

    for step in range(chips):
        remote(
            give.at[step], near.at[step], near_sems.at[4 * step], near_sems.at[4 * step + 1], partner
        ).wait_send()
    for step in range(chips - 1):
        device = order[step] * pair + core
        for i, lanes in enumerate((slice(0, breadth), side_block)):
            sent = remote(
                mixed.at[step, :, :, lanes],
                far.at[step, :, :, lanes],
                far_sems.at[step, len(far_groups) + i],
                far_sems.at[step, 0],
                (w, device),
            )
            if i == 0:
                sent.wait_send()
            else:
                pl.when(has_outer(device))(sent.wait_send)
    remote(
        field.at[0, :, (1 - core) * (tiles - 1), shifted(slice(0, height)), :],
        field_inner,
        col_sems.at[len(swaps)],
        col_sems.at[0],
        partner,
    ).wait_send()
    fixed_column().wait_send()
    given_column().wait_send()
    pl.when(has_outer(n))(outer_column().wait_send)
    left(has_row, fixed_both, given_both, field_both)

    for side in (0, 1):
        @pl.when(has_row[side])
        def _():
            late_row(1 - side).wait_recv()
            for k in range(layers):
                field[0, k, :, halo_beyond[side], :] = field_late[side, k]

    ends = (all_blocks[0], all_blocks[-1])
    for step in range(final_step):
        for b in ends:
            forward(step, Block(b))
    arrived(has_row, given_both)
    for b in ends:
        mask_given(b)
    for b in (all_blocks[1], all_blocks[-2]):
        last_forward(Block(b), keep_grad(final_step, Block(b)))
    last_forward(Pair(-HALF), keep_grad(final_step, Pair(-HALF)))
    for b in (*all_blocks[:2], *all_blocks[-2:]):
        turn_weights(b)

    for step in range(final_step, -1, -1):
        for b in all_blocks[1:-1]:
            back(step, Block(b))
    for side in (0, 1):
        receive_round(side)
    for step in range(final_step, -1, -1):
        back(step, Pair(-2 * step))

    left(has_row, round_both)


def body(group_wide, group, slots, owner, row_v, col_v, land_sea, layer_class, speed, final, deposit):
    layers, height, breadth = final.shape
    chips = group // 2
    hops = max(chips - 1, 1)
    f32 = jnp.float32
    extended = height + 2 * ROWS
    padded = extended + 2 * ROWS
    width = breadth + LANES
    tiles = width // LANES
    dma = pltpu.SemaphoreType.DMA
    vmem = pl.BlockSpec(memory_space=pltpu.VMEM)
    hbm = pl.BlockSpec(memory_space=pltpu.HBM)
    return pl.pallas_call(
        functools.partial(kernel, group_wide, group),
        out_shape=pltpu.VMEM(final.shape, f32),
        in_specs=[hbm] * 9,
        out_specs=vmem,
        scratch_shapes=[
            pltpu.SMEM(owner.shape, owner.dtype),
            pltpu.SMEM(layer_class.shape, layer_class.dtype),
            pltpu.SMEM(speed.shape, speed.dtype),
            pltpu.VMEM(land_sea.shape, land_sea.dtype),
            pltpu.VMEM((3, extended, width), f32),
            pltpu.VMEM((3, height, LANES), f32),
            pltpu.VMEM((layers + 1, extended, width), f32),
            pltpu.VMEM((layers + 1, height, LANES), f32),
            pltpu.VMEM((height, LANES), f32),
            pltpu.VMEM((height, LANES), f32),
            pltpu.VMEM((chips, layers, height, width), f32),
            pltpu.VMEM((chips, layers, height, width), f32),
            pltpu.VMEM((chips, layers, height, width), f32),
            pltpu.VMEM((hops, layers, height, width), f32),
            pltpu.VMEM((hops, layers, height, width), f32),
            pltpu.VMEM((STEPS, layers, tiles, padded, LANES), f32),
            pltpu.VMEM((layers, height, LANES), f32),
            pltpu.VMEM((layers, height, LANES), f32),
            pltpu.VMEM((2, layers, tiles, HALF, LANES), f32),
            pltpu.VMEM((STEPS, layers, tiles, extended, LANES), f32),
            pltpu.VMEM((STEPS, layers, tiles, padded, LANES), f32),
            pltpu.VMEM((4, tiles, padded, LANES), f32),
            pltpu.VMEM((4, tiles, extended, LANES), f32),
            pltpu.VMEM((4, tiles, extended, LANES), f32),
            pltpu.VMEM((4, tiles, extended, LANES), f32),
            pltpu.VMEM((tiles, extended, LANES), f32),
            pltpu.VMEM((tiles, extended, LANES), f32),
            pltpu.VMEM((layers, tiles, extended, LANES), f32),
            pltpu.VMEM((tiles, extended, LANES), f32),
            pltpu.VMEM((2, layers, tiles, HALF, LANES), f32),
            pltpu.VMEM((2, layers, tiles, HALF, LANES), f32),
            dma((5,)),
            dma((2, chips)),
            dma((4 * (chips - 1) + 2,)),
            dma((hops, 17 + 2)),
            dma((2, 4)),
            dma((2, 3)),
            dma((6,)),
            dma((2, 2)),
            dma((2,)),
            dma((2, 2)),
        ],
        compiler_params=pltpu.CompilerParams(
            collective_id=0,
            has_side_effects=True,
            vmem_limit_bytes=VMEM_BYTES - final.size * final.dtype.itemsize,
        ),
    )(owner, layer_class, speed, slots, row_v, col_v, land_sea, final, deposit)


def solution(mesh):
    in_specs = (
        P("narrow", None, "wide", None),
        P(),
        P("wide", "narrow"),
        P("wide", "narrow"),
        P("wide", "narrow"),
        P(),
        P(),
        P(None, "wide", "narrow"),
        P("wide", "narrow"),
    )
    out_specs = P(None, "wide", "narrow")
    return jax.shard_map(
        functools.partial(body, mesh.shape["wide"], mesh.shape["narrow"]),
        mesh=mesh,
        in_specs=in_specs,
        out_specs=out_specs,
        check_vma=False,
    )
```
